32 devices in a mesh: dp: 16 (over z, y, core), tensor: 2 (over x).
Axes of the slice: x: 2, y: 2, z: 4, core: 2. Of those that a mesh axis runs over, the one named last changes fastest.
Arguments:
- attn_out: bfloat16 [12288, 2048], P('dp', 'tensor'), may hold values from -6 to 6
- out_proj_t: bfloat16 [4096, 2048], P(None, 'tensor'), may hold values from -0.09375 to 0.09375
- grad_out: bfloat16 [12288, 4096], P('dp', 'tensor'), may hold values from -6 to 6
- read_weights: float32 [12288, 16], P('dp'), may hold values from 0 to 0.0026041667
- memory_gate: float32 [256, 16], P('dp'), may hold values from -0.2 to 1
- write_pos: int32 [16, 16], P('dp'), may hold values from 0 to 767, as said below
Outputs:
- grad_attn_out: bfloat16 [12288, 2048], P('dp', 'tensor')
- grad_out_proj_t: float32 [4096, 2048], P('dp', 'tensor')
- grad_memory: float32 [256, 4096], P('dp', 'tensor')
The draws below stay inside these ranges and needn't reach their ends.
Inputs may be any that keep to these rules, and one draw needn't show every extreme that they name: `write_pos`: the 16 positions of one segment are distinct.
All inputs are finite; a program needn't handle non-finite values.
Results may differ from the reference program's by a relative error of at most 0.0034.
Values may be sent and summed in bfloat16 or wider, within the bound.
A program may use at most 64 MiB of HBM per device.

```python
import jax
import jax.numpy as jnp
from jax import lax

D = 4096
MEM = 16
SEG = 768
SEGMENT_COUNT = 16
HD = 2048
TOKENS = 12288


def draw_memory_gate(key, part):
    share = 0.5
    gradual_decay = jax.random.uniform(jax.random.fold_in(key, 1), (1, MEM)) < share
    gradual_decay_rate = jnp.exp(-jax.random.uniform(jax.random.fold_in(key, 2), (SEGMENT_COUNT, MEM), jnp.float32, 0.2, 1.5) / SEGMENT_COUNT)
    quick_decay_rate = jax.random.uniform(jax.random.fold_in(key, 3), (SEGMENT_COUNT, MEM), jnp.float32, 0.05, 0.5)
    sudden_spike = jax.random.uniform(jax.random.fold_in(key, 4), (SEGMENT_COUNT, 1)) < 3.0 / SEGMENT_COUNT
    decay_rates = jnp.where(gradual_decay, gradual_decay_rate, quick_decay_rate) * jnp.where(sudden_spike, 0.6, 1.0)
    eye = jnp.eye(MEM, dtype=jnp.float32)
    spread = jnp.clip(jax.random.normal(jax.random.fold_in(key, 5), (SEGMENT_COUNT, MEM, MEM)) * 0.04, -0.2, 0.2)
    gates = spread * (1.0 - eye) + decay_rates[:, :, None] * eye
    return gates.reshape(SEGMENT_COUNT * MEM, MEM).astype(jnp.float32)


def draw_write_pos(key, part):
    keys = jax.random.split(jax.random.fold_in(key, 7), SEGMENT_COUNT)
    picks = jax.vmap(lambda single: jax.random.permutation(single, SEG)[:MEM])(keys)
    return picks.astype(jnp.int32)


def spiked(drawn, stream_key, source, target, parts, factor):
    def block_of(position):
        return (jnp.arange(drawn.shape[position]) // (drawn.shape[position] // parts)).reshape((-1,) + (1,) * (drawn.ndim - 1 - position))

    one_side = jax.random.permutation(stream_key, parts)[block_of(target)]
    second = (block_of(target) + parts // 2) % parts
    return jnp.where((block_of(source) == one_side) | (block_of(source) == second), factor * drawn, drawn)


def levels(rng, dims, cuts, low, high):
    def one(dim, shards_of):
        steps = jax.random.uniform(jax.random.fold_in(jax.random.fold_in(rng, 6), dim), (shards_of,), jnp.float32, low / len(cuts), high / len(cuts))
        return jnp.repeat(jnp.exp(steps), dims[dim] // shards_of).reshape((-1,) + (1,) * (len(dims) - dim - 1))

    factor_of = one(*cuts[0])
    for cut in cuts[1:]:
        factor_of = factor_of * one(*cut)
    return factor_of


def noise(own_key, extent, scale, reach, pieces=(), kind=jnp.bfloat16):
    drawn = scale * jax.random.normal(own_key, extent, jnp.float32)
    if pieces:
        drawn = drawn * levels(own_key, extent, pieces, -0.22, 0.18)
    return jnp.clip(drawn, -reach, reach).astype(kind)


def heavy_noise(own_key, shape, width, most, pieces, heavy, held_as=jnp.bfloat16):
    array = width * jax.random.normal(own_key, shape, jnp.float32)
    if pieces:
        array = array * levels(own_key, shape, pieces, -0.22, 0.18)
    return jnp.clip(spiked(array, jax.random.fold_in(own_key, 3), *heavy), -most, most).astype(held_as)


def setup_inputs(seed: int = 0) -> dict:
    seeds = jax.random.split(jax.random.key(seed), 7)
    attn_out = noise(seeds[0], (TOKENS, HD), 1.0, 6.0, ((0, 16), (1, 2)))
    out_proj_t = noise(seeds[1], (D, HD), D ** -0.5, 0.09375, ((1, 2),))
    grad_out = heavy_noise(seeds[2], (TOKENS, D), 1.0, 6.0, ((0, 16), (1, 2)), (0, 1, 16, 2.0))
    read_weights = jnp.clip(0.0026041667 * jax.random.uniform(seeds[3], (TOKENS, MEM), jnp.float32) ** levels(seeds[3], (TOKENS, MEM), ((0, 16),), -0.2, 0.2), 0.0, 0.0026041667)
    memory_gate = draw_memory_gate(jax.random.fold_in(seeds[6], 71), 0)
    write_pos = draw_write_pos(jax.random.fold_in(seeds[6], 71), 0)
    return {"attn_out": attn_out, "out_proj_t": out_proj_t, "grad_out": grad_out, "read_weights": read_weights, "memory_gate": memory_gate, "write_pos": write_pos}


def reference(attn_out, out_proj_t, grad_out, read_weights, memory_gate, write_pos):
    high = lax.Precision.HIGHEST
    dy = grad_out.astype(jnp.float32).reshape(SEGMENT_COUNT, SEG, D)
    reads = read_weights.reshape(SEGMENT_COUNT, SEG, MEM)
    gates = memory_gate.reshape(SEGMENT_COUNT, MEM, MEM)
    local = jnp.einsum('stm,std->smd', reads, dy, precision=high)

    def sweep(carry, inputs):
        gate, term = inputs
        fresh = jnp.dot(gate.T, carry, precision=high, preferred_element_type=jnp.float32) + term
        return fresh, (fresh, carry)

    start = jnp.zeros((MEM, D), jnp.float32)
    _, (grad_mem, after) = lax.scan(sweep, start, (gates, local), reverse=True)
    places = jnp.arange(SEG, dtype=jnp.int32)
    onehot = (places[None, :, None] == write_pos[:, None, :]).astype(jnp.float32)
    written = jnp.einsum('stm,smd->std', onehot, after, precision=high)
    grad_z = (dy + written).astype(jnp.bfloat16).reshape(TOKENS, D)
    grad_attn = jnp.dot(grad_z, out_proj_t, preferred_element_type=jnp.float32).astype(jnp.bfloat16)
    grad_weight = lax.dot_general(grad_z, attn_out, (((0,), (0,)), ((), ())), preferred_element_type=jnp.float32)
    return grad_attn, grad_weight, grad_mem.reshape(SEGMENT_COUNT * MEM, D)
```

```python
import functools

import jax
import jax.numpy as jnp
from jax import lax
from jax.experimental import pallas as pl
from jax.experimental.pallas import tpu as pltpu
from jax.sharding import PartitionSpec as P

MESH = pl.DeviceIdType.MESH
F32 = jnp.float32
BF16 = jnp.bfloat16
EARLY = 2


def split3(a):
    hi = a.astype(BF16)
    rest = a - hi.astype(F32)
    mid = rest.astype(BF16)
    low = (rest - mid.astype(F32)).astype(BF16)
    return jnp.concatenate([hi, mid, low], axis=0)


def tdot(a, b):
    return lax.dot_general(a, b, (((0,), (0,)), ((), ())), preferred_element_type=F32)


def plan(nu, ns, early):
    steps = []
    for u in range(nu):
        lead = u < nu // 2
        own = 2.0 + 0.2 * u if lead else (3.05 + 0.05 * (u - nu // 2) if u < nu - 2 else 5.15 + 0.05 * (u + 2 - nu))
        steps.append((own, "own", u))
        if u < early:
            steps.append((early + 0.1 + 0.25 * u, "prep", u))
            arrived = early + 0.2 + 0.25 * u
        else:
            arrived = u + 1.0
        steps.append((arrived, "other", u))
        if u % 2:
            steps.append((max(own + 0.01, 3.05 + 0.67 * (u - 1)), "own_out", u))
            steps.append((max(arrived + 0.01, 3.7 + 0.66 * (u - 1)), "other_out", u))
        if (u + 1) % (2 * ns) == 0:
            last = u == nu - 1
            steps.append((arrived + (0.1 if last else 1.5), "attn", u // (2 * ns)))
    steps.append((4.2, "own_attn", 0))
    steps.append((4.25, "memory", 0))
    return [step[1:] for step in sorted(steps, key=lambda step: step[0])]


def kernel(
    n, early, attn_hbm, w_hbm, g_hbm, rwt, gate, wpos, out_attn, out_w, out_mem,
    g, attn, w, attn_p, za, zb, zp, zpx, acc, onehot, mask, grow, rows, rows_x, local, after,
    gpad, grecv, lrecv, asend, arecv, ysend, yrecv, kept, zsend, zrecv, mine,
    g_sem, attn_sem, w_sem, xa_s, xa_r, xb_s, xb_r, gt_s, gt_r, l_s, l_r, a_s, a_r, r_s, r_r, t_s, t_r,
    p_s, p_r, q_s, q_r, y_s, y_r, z_s, z_r,
):
    d = lax.axis_index("dp")
    t = lax.axis_index("tensor")
    c = lax.rem(d, 2)
    y = lax.rem(d // 2, 2)
    z = d // 4
    nz = n // 4
    seg, half = g.shape
    hd = attn.shape[1]
    slots = rwt.shape[0]
    bw = 2 * half // n
    lw = half // n
    zh = nz // 2
    sub = mask.shape[1]
    ns = bw // sub
    nu = 2 * zh * ns
    oh = 1 - t
    pd = d + 1 - 2 * c
    partner = (pd, t)
    xpeer = (d, oh)
    ypeer = (d + 2 - 4 * y, t)
    tile = 256

    def remote(src, dst, ss, rs, dev):
        return pltpu.make_async_remote_copy(
            src_ref=src, dst_ref=dst, send_sem=ss, recv_sem=rs, device_id=dev, device_id_type=MESH
        )

    def peer(o):
        return lax.rem(d + o, n)

    barrier = pltpu.get_barrier_semaphore()
    for o in range(1, n):
        pl.semaphore_signal(barrier, inc=1, device_id=(peer(o), t), device_id_type=MESH)
    pl.semaphore_signal(barrier, inc=1, device_id=xpeer, device_id_type=MESH)
    pl.semaphore_signal(barrier, inc=1, device_id=(pd, oh), device_id_type=MESH)

    gcopy = pltpu.make_async_copy(g_hbm, g, g_sem)
    gcopy.start()
    attncopy = pltpu.make_async_copy(attn_hbm, attn, attn_sem)
    attncopy.start()
    gpad[...] = jnp.zeros_like(gpad)
    gpad[:, :slots] = gate[...].T
    three = split3(rwt[...])
    place_of = lax.broadcasted_iota(jnp.int32, (seg, slots), 0)
    hit = jnp.where(place_of == wpos[...], 1.0, 0.0)
    onehot[...] = hit.astype(BF16)
    mask[...] = jnp.broadcast_to(jnp.sum(hit, axis=1, keepdims=True), mask.shape)
    pl.semaphore_wait(barrier, n + 1)

    def is_other(u):
        return u % 2 == 0

    def level(h, r):
        return r + h * (zh - 1 - 2 * r)

    def cols(h, u, par):
        yd = 1 - y if is_other(u) else y
        j = 2 * level(h, u // (2 * ns)) + yd
        piece = u % (2 * ns) // 2
        return pl.ds(pl.multiple_of((2 * j + par) * bw + piece * sub, sub), sub)

    def wide(h, r):
        return pl.multiple_of(4 * level(h, r) * bw, 4 * bw)

    xa, xb = [], []
    for u in range(nu):
        mine_at, part_at = cols(t, u, c), cols(t, u, 1 - c)
        src = g_hbm if u < early else za
        xa.append(remote(src.at[:, mine_at], zb.at[:, mine_at], xa_s.at[u], xa_r.at[u], xpeer))
        if u < early:
            xb.append(remote(src.at[:, part_at], zb.at[:, part_at], xb_s.at[u], xb_r.at[u], xpeer))
        else:
            xb.append(remote(src.at[:, part_at], zpx.at[u], xb_s.at[u], xb_r.at[u], (pd, oh)))
    for u in range(early):
        xb[u].start()
        xa[u].start()

    grecv[0] = gpad[...]
    gcopies = [remote(gpad, grecv.at[o], gt_s.at[o], gt_r.at[o], (peer(o), t)) for o in range(1, n)]
    for copy in gcopies:
        copy.start()
    wcopy = pltpu.make_async_copy(w_hbm, w, w_sem)
    wcopy.start()
    tcopy = remote(attn_hbm, attn_p, t_s, t_r, partner)
    tcopy.start()
    gcopy.wait()

    def local_step(i, _):
        at = pl.ds(pl.multiple_of(i * tile, tile), tile)
        r = jnp.dot(three, g[:, at], preferred_element_type=F32)
        local[:, at] = r[:slots] + r[slots : 2 * slots] + r[2 * slots :]
        return 0

    lax.fori_loop(0, half // tile, local_step, 0)

    def slab(o):
        return pl.ds(pl.multiple_of(peer(o) * lw, lw), lw)

    lcopies = [
        remote(local.at[:, slab(o)], lrecv.at[o], l_s.at[o], l_r.at[o], (peer(o), t)) for o in range(1, n)
    ]
    for copy in lcopies:
        copy.start()
    lrecv[0] = local[:, slab(0)]

    def row_step(i, _):
        at = pl.ds(pl.multiple_of(i * tile, tile), tile)
        grow[:, at] = tdot(onehot[...], g[:, at])
        return 0

    lax.fori_loop(0, half // tile, row_step, 0)
    for copy in gcopies + lcopies:
        copy.wait_recv()

    def acopy(o, target):
        return remote(asend.at[o], arecv.at[o], a_s.at[o], a_r.at[o], (target, t))

    def sweep(i, carry):
        s = n - 1 - i
        slot = lax.rem(d - s + n, n)
        target = lax.rem(s - d + n, n)
        asend[target] = carry
        gates = grecv[slot]
        fresh = lrecv[slot]
        for k in range(slots):
            fresh = fresh + gates[:, k : k + 1] * carry[k : k + 1, :]

        @pl.when(target != 0)
        def _():
            acopy(target, s).start()

        return fresh

    lax.fori_loop(0, n, sweep, jnp.zeros((slots, lw), F32))
    acopies = [acopy(o, peer(o)) for o in range(1, n)]
    for o in range(n):
        if o:
            acopies[o - 1].wait_recv()
        src = lax.rem(d - o + n, n)
        at = pl.ds(pl.multiple_of(src * lw, lw), lw)
        got = arecv[o] if o else asend[0]
        after[:, at] = got
        rows[:, at] = (grow[:, at] + got).astype(BF16)
    rows_at = pl.ds(wide(t, 0), 4 * bw)
    rcopy = remote(rows.at[:, rows_at], rows_x.at[:, rows_at], r_s, r_r, xpeer)
    rcopy.start()

    def fix(src, new_rows, dst, at):
        picked = jnp.dot(onehot[...], new_rows[:, at], preferred_element_type=F32)
        dst[:, at] = jnp.where(mask[...] > 0.5, picked, src[:, at].astype(F32)).astype(BF16)

    pcopies = [
        remote(za.at[:, cols(t, u, 1 - c)], zp.at[u], p_s.at[u], p_r.at[u], partner) for u in range(nu)
    ]
    qcopies = []
    for u in range(nu):
        if u < early:
            qcopies.append(remote(zb.at[:, cols(oh, u, 1 - c)], zpx.at[u], q_s.at[u], q_r.at[u], partner))
        else:
            qcopies.append(remote(zpx.at[u], zb.at[:, cols(oh, u, c)], q_s.at[u], q_r.at[u], partner))

    def fix_own(u):
        fix(g, rows, za, cols(t, u, 1 - c))
        fix(g, rows, za, cols(t, u, c))
        pcopies[u].start()
        if u >= early:

            @pl.when(c == 0)
            def _():
                xa[u].start()
                xb[u].start()

            @pl.when(c == 1)
            def _():
                xb[u].start()
                xa[u].start()

    for u in [*range(early, min(early + 2, nu)), *range(early), *range(early + 2, nu)]:
        fix_own(u)

    ycopies, ncopies = {}, []

    def slot_of(own, u):
        return (0 if own else nu // 2) + u // 2

    def grad_block(own, u):
        slot = slot_of(own, u)
        zr, zq, at = (za, zp, cols(t, u, c)) if own else (zb, zpx, cols(oh, u, c))

        def step(m, _):
            ht = pl.ds(pl.multiple_of(m * tile, tile), tile)
            r = tdot(zr[:, at], attn[:, ht]) + tdot(zq[u], attn_p[:, ht])
            if is_other(u):
                ysend[slot, :, ht] = r.astype(BF16)
            else:
                kept[slot, :, ht] = r
            return 0

        lax.fori_loop(0, hd // tile, step, 0)
        if is_other(u):
            copy = remote(ysend.at[slot], yrecv.at[slot], y_s.at[slot], y_r.at[slot], ypeer)
            copy.start()
            ycopies[slot] = copy

    def to_owner(own, u):
        slot = slot_of(own, u)
        piece = u % (2 * ns) // 2
        h = t if own else oh
        zd = zh * h + level(h, u // (2 * ns))
        ycopies[slot].wait_recv()
        at_home = zd == z

        @pl.when(at_home)
        def _():
            mine[piece] = kept[slot] + yrecv[slot].astype(F32)

        @pl.when(jnp.logical_not(at_home))
        def _():
            o = lax.rem(zd - z + nz, nz)
            zsend[slot] = (kept[slot] + yrecv[slot].astype(F32)).astype(BF16)
            remote(
                zsend.at[slot],
                zrecv.at[o, piece],
                z_s.at[slot],
                z_r.at[o, piece],
                (zd * 4 + 2 * y + c, t),
            ).start()

        ncopies.append((at_home, slot))

    def own_attn():
        wcopy.wait()

        def step(m, _):
            at = pl.ds(pl.multiple_of(m * tile, tile), tile)
            k = pl.ds(pl.multiple_of(t * half, half), half)
            acc[:, at] = jnp.dot(za[...], w[k, at], preferred_element_type=F32)
            return 0

        lax.fori_loop(0, hd // tile, step, 0)

    def other_attn(r):
        from_at = wide(oh, r)
        last = r == zh - 1
        for u in range(2 * ns * r, 2 * ns * (r + 1)):
            if u >= early:
                qcopies[u].wait_recv()

        def step(m, _):
            at = pl.ds(pl.multiple_of(m * tile, tile), tile)
            k = pl.ds(pl.multiple_of(oh * half + from_at, 4 * bw), 4 * bw)
            total = acc[:, at] + jnp.dot(
                zb[:, pl.ds(from_at, 4 * bw)], w[k, at], preferred_element_type=F32
            )
            if last:
                out_attn[:, at] = total.astype(BF16)
            else:
                acc[:, at] = total
            return 0

        lax.fori_loop(0, hd // tile, step, 0)

    def memory():
        gates = gpad[...]

        def step(i, _):
            at = pl.ds(pl.multiple_of(i * tile, tile), tile)
            fresh = local[:, at]
            carry = after[:, at]
            for k in range(slots):
                fresh = fresh + gates[:, k : k + 1] * carry[k : k + 1, :]
            out_mem[:, at] = fresh
            return 0

        lax.fori_loop(0, half // tile, step, 0)

    waited = set()

    def once(name, copy):
        if name not in waited:
            waited.add(name)
            copy.wait_recv()

    attncopy.wait()
    for kind, u in plan(nu, ns, early):
        if kind == "own":
            once("attn", tcopy)
            pcopies[u].wait_recv()
            grad_block(True, u)
        elif kind == "prep":
            once("rows", rcopy)
            xb[u].wait_recv()
            fix(zb, rows_x, zb, cols(oh, u, 1 - c))
            qcopies[u].start()
            xa[u].wait_recv()
            fix(zb, rows_x, zb, cols(oh, u, c))
        elif kind == "other":
            if u < early:
                qcopies[u].wait_recv()
            else:
                xa[u].wait_recv()
                xb[u].wait_recv()
                qcopies[u].start()
            grad_block(False, u)
        elif kind == "own_out":
            to_owner(True, u)
        elif kind == "other_out":
            to_owner(False, u)
        elif kind == "own_attn":
            own_attn()
        elif kind == "attn":
            other_attn(u)
        else:
            memory()

    for piece in range(ns):
        total = mine[piece]
        for o in range(1, nz):
            remote(
                zrecv.at[o, piece], zrecv.at[o, piece], z_s.at[0], z_r.at[o, piece], ypeer
            ).wait_recv()
            total = total + zrecv[o, piece].astype(F32)
        out_w[pl.ds(piece * sub, sub), :] = total

    sent = xa + xb + gcopies + lcopies + acopies + pcopies + qcopies + list(ycopies.values())
    for copy in sent + [tcopy, rcopy]:
        copy.wait_send()
    for at_home, slot in ncopies:

        @pl.when(jnp.logical_not(at_home))
        def _():
            remote(
                zsend.at[slot], zrecv.at[0, 0], z_s.at[slot], z_r.at[0, 0], ypeer
            ).wait_send()


def fused(n, attn_out, out_proj_t, grad_out, read_weights, memory_gate, write_pos):
    seg, half = grad_out.shape
    hd = attn_out.shape[1]
    slots = write_pos.shape[1]
    depth = out_proj_t.shape[0]
    bw, lw, nz = depth // n, half // n, n // 4
    sub = 128
    ns = bw // sub
    nu = nz * ns
    early = EARLY
    V = pltpu.VMEM
    D = pltpu.SemaphoreType.DMA
    vmem = pl.BlockSpec(memory_space=pltpu.VMEM)
    return pl.pallas_call(
        functools.partial(kernel, n, early),
        out_shape=(
            jax.ShapeDtypeStruct((seg, hd), BF16),
            jax.ShapeDtypeStruct((bw, hd), F32),
            jax.ShapeDtypeStruct((slots, half), F32),
        ),
        in_specs=[pl.BlockSpec(memory_space=pl.ANY)] * 3 + [vmem] * 3,
        out_specs=(vmem, vmem, vmem),
        scratch_shapes=[
            V((seg, half), BF16),
            V((seg, hd), BF16),
            V((depth, hd), BF16),
            V((seg, hd), BF16),
            V((seg, half), BF16),
            V((seg, half), BF16),
            V((nu, seg, sub), BF16),
            V((nu, seg, sub), BF16),
            V((seg, hd), F32),
            V((seg, slots), BF16),
            V((seg, sub), F32),
            V((slots, half), F32),
            V((slots, half), BF16),
            V((slots, half), BF16),
            V((slots, half), F32),
            V((slots, half), F32),
            V((slots, 128), F32),
            V((n, slots, 128), F32),
            V((n, slots, lw), F32),
            V((n, slots, lw), F32),
            V((n, slots, lw), F32),
            V((nu, sub, hd), BF16),
            V((nu, sub, hd), BF16),
            V((nu, sub, hd), F32),
            V((nu, sub, hd), BF16),
            V((nz, ns, sub, hd), BF16),
            V((ns, sub, hd), F32),
            D,
            D,
            D,
            D((nu,)),
            D((nu,)),
            D((nu,)),
            D((nu,)),
            D((n,)),
            D((n,)),
            D((n,)),
            D((n,)),
            D((n,)),
            D((n,)),
            D,
            D,
            D,
            D,
            D((nu,)),
            D((nu,)),
            D((nu,)),
            D((nu,)),
            D((nu,)),
            D((nu,)),
            D((nu,)),
            D((nz, ns)),
        ],
        compiler_params=pltpu.CompilerParams(
            collective_id=0, has_side_effects=True, vmem_limit_bytes=62 * 1024 * 1024
        ),
    )(attn_out, out_proj_t, grad_out, read_weights.T, memory_gate, write_pos)


def plain(attn_out, out_proj_t, grad_out, read_weights, memory_gate, write_pos):
    high = lax.Precision.HIGHEST
    seg_len = attn_out.shape[0]
    slots = write_pos.shape[1]
    gate_at_step = memory_gate.T
    dy_cols = grad_out.astype(jnp.float32)
    local = jnp.dot(read_weights.T, dy_cols, precision=high, preferred_element_type=jnp.float32)
    all_gates, all_terms = (
        lax.all_gather(gate_at_step, "dp", axis=0, tiled=True),
        lax.all_gather(local, "dp", axis=0, tiled=True),
    )
    count = lax.axis_size("dp")
    mine = lax.axis_index("dp")

    def sweep(step, carry):
        which = (count - 1 - step).astype(jnp.int32)
        gate = lax.dynamic_slice_in_dim(all_gates, which * slots, slots, 0)
        term = lax.dynamic_slice_in_dim(all_terms, which * slots, slots, 0)
        fresh = jnp.dot(gate, carry, precision=high, preferred_element_type=jnp.float32) + term
        return jnp.where(which > mine, fresh, carry)

    after = lax.fori_loop(0, count, sweep, jnp.zeros_like(local))
    grad_memory = (
        jnp.dot(gate_at_step, after, precision=high, preferred_element_type=jnp.float32) + local
    )
    places = jnp.arange(seg_len, dtype=jnp.int32)
    onehot = (places[:, None] == write_pos[0][None, :]).astype(jnp.float32)
    written = jnp.dot(onehot, after, precision=high, preferred_element_type=jnp.float32)
    grad_z = (dy_cols + written).astype(jnp.bfloat16)
    full_z = lax.all_gather(grad_z, "tensor", axis=1, tiled=True)
    grad_attn = jnp.dot(full_z, out_proj_t, preferred_element_type=jnp.float32).astype(jnp.bfloat16)
    term = lax.dot_general(
        full_z, attn_out, (((0,), (0,)), ((), ())), preferred_element_type=jnp.float32
    )
    grad_weight = lax.psum_scatter(term, "dp", scatter_dimension=0, tiled=True)
    return (grad_attn, grad_weight, grad_memory)


def solution(mesh):
    n = mesh.shape["dp"]
    parts = mesh.shape["tensor"]

    def body(attn_out, out_proj_t, grad_out, read_weights, memory_gate, write_pos):
        half, hd = grad_out.shape[1], attn_out.shape[1]
        fits = (
            parts == 2
            and n // 4 == 4
            and half % (n * 128) == 0
            and half % 256 == 0
            and hd % 256 == 0
            and out_proj_t.shape[0] <= 4096
        )
        args = (attn_out, out_proj_t, grad_out, read_weights, memory_gate, write_pos)
        return fused(n, *args) if fits else plain(*args)

    return jax.shard_map(
        body,
        mesh=mesh,
        in_specs=(
            P("dp", "tensor"),
            P(None, "tensor"),
            P("dp", "tensor"),
            P("dp", None),
            P("dp", None),
            P("dp", None),
        ),
        out_specs=(P("dp", "tensor"), P("dp", "tensor"), P("dp", "tensor")),
        check_vma=False,
    )
```

```python
import functools

import jax
import jax.numpy as jnp
from jax import lax
from jax.experimental import pallas as pl
from jax.experimental.pallas import tpu as pltpu
from jax.sharding import PartitionSpec as P

MESH = pl.DeviceIdType.MESH
F32 = jnp.float32
BF16 = jnp.bfloat16
EARLY = 2


def split3(a):
    hi = a.astype(BF16)
    rest = a - hi.astype(F32)
    mid = rest.astype(BF16)
    low = (rest - mid.astype(F32)).astype(BF16)
    return jnp.concatenate([hi, mid, low], axis=0)


def tdot(a, b):
    return lax.dot_general(a, b, (((0,), (0,)), ((), ())), preferred_element_type=F32)


def plan(nu, ns, early):
    steps = []
    for u in range(nu):
        lead = u < nu // 2
        own = 2.0 + 0.2 * u if lead else (3.05 + 0.05 * (u - nu // 2) if u < nu - 2 else 5.15 + 0.05 * (u + 2 - nu))
        steps.append((own, "own", u))
        if u < early:
            steps.append((early + 0.1 + 0.25 * u, "prep", u))
            arrived = early + 0.2 + 0.25 * u
        else:
            arrived = u + 1.0
        steps.append((arrived, "other", u))
        if u % 2:
            sent = max(own + 0.01, 3.05 + 0.67 * (u - 1))
            steps.append((sent, "own_out", u))
            steps.append((sent + 0.9, "own_pass", u))
            sent = max(arrived + 0.01, 3.7 + 0.66 * (u - 1))
            if u < nu - 1:
                steps.append((sent, "other_out", u))
            steps.append((sent + 0.9, "other_pass", u))
        if (u + 1) % (2 * ns) == 0:
            last = u == nu - 1
            steps.append((arrived + (0.1 if last else 1.5), "attn", u // (2 * ns)))
    steps.append((4.2, "own_attn", 0))
    steps.append((4.25, "memory", 0))
    return [step[1:] for step in sorted(steps, key=lambda step: step[0])]


def kernel(
    n, early, attn_hbm, w_hbm, g_hbm, rwt_hbm, gate_hbm, wpos_hbm, out_attn, out_w, out_mem,
    rwt, gate, wpos, g, attn, w, attn_p, za, zb, zp, zpx, acc, onehot, mask, grow, rows, rows_x, local, after,
    gpad, grecv, lrecv, asend, arecv, ysend, yrecv, kept, zsend, zpass, zrecv, mine,
    small_sem, g_sem, attn_sem, w_sem, xa_s, xa_r, xb_s, xb_r, gt_s, gt_r, l_s, l_r, a_s, a_r, r_s, r_r, t_s, t_r,
    p_s, p_r, q_s, q_r, y_s, y_r, z_s, v_r, z_r,
):
    d = lax.axis_index("dp")
    t = lax.axis_index("tensor")
    c = lax.rem(d, 2)
    y = lax.rem(d // 2, 2)
    z = d // 4
    nz = n // 4
    seg, half = g.shape
    hd = attn.shape[1]
    slots = rwt.shape[0]
    bw = 2 * half // n
    lw = half // n
    zh = nz // 2
    sub = mask.shape[1]
    ns = bw // sub
    nu = 2 * zh * ns
    oh = 1 - t
    pd = d + 1 - 2 * c
    partner = (pd, t)
    xpeer = (d, oh)
    ypeer = (d + 2 - 4 * y, t)
    tile = 256

    def remote(src, dst, ss, rs, dev):
        return pltpu.make_async_remote_copy(
            src_ref=src, dst_ref=dst, send_sem=ss, recv_sem=rs, device_id=dev, device_id_type=MESH
        )

    def peer(o):
        return lax.rem(d + o, n)

    barrier = pltpu.get_barrier_semaphore()
    for o in range(1, n):
        pl.semaphore_signal(barrier, inc=1, device_id=(peer(o), t), device_id_type=MESH)
    pl.semaphore_signal(barrier, inc=1, device_id=xpeer, device_id_type=MESH)
    pl.semaphore_signal(barrier, inc=1, device_id=(pd, oh), device_id_type=MESH)

    smalls = [
        pltpu.make_async_copy(src, dst, small_sem.at[i])
        for i, (src, dst) in enumerate(((rwt_hbm, rwt), (gate_hbm, gate), (wpos_hbm, wpos)))
    ]
    for copy in smalls:
        copy.start()
    gcopy = pltpu.make_async_copy(g_hbm, g, g_sem)
    gcopy.start()
    attncopy = pltpu.make_async_copy(attn_hbm, attn, attn_sem)
    attncopy.start()
    for copy in smalls:
        copy.wait()
    gpad[...] = jnp.zeros_like(gpad)
    gpad[:, :slots] = gate[...].T
    three = split3(rwt[...])
    place_of = lax.broadcasted_iota(jnp.int32, (seg, slots), 0)
    hit = jnp.where(place_of == wpos[...], 1.0, 0.0)
    onehot[...] = hit.astype(BF16)
    mask[...] = jnp.broadcast_to(jnp.sum(hit, axis=1, keepdims=True), mask.shape)
    pl.semaphore_wait(barrier, n + 1)

    def is_other(u):
        return u % 2 == 0

    def level(h, r):
        return r + h * (zh - 1 - 2 * r)

    def cols(h, u, par):
        yd = 1 - y if is_other(u) else y
        j = 2 * level(h, u // (2 * ns)) + yd
        piece = u % (2 * ns) // 2
        return pl.ds(pl.multiple_of((2 * j + par) * bw + piece * sub, sub), sub)

    def wide(h, r):
        return pl.multiple_of(4 * level(h, r) * bw, 4 * bw)

    xa, xb = [], []
    for u in range(nu):
        mine_at, part_at = cols(t, u, c), cols(t, u, 1 - c)
        src = g_hbm if u < early else za
        xa.append(remote(src.at[:, mine_at], zb.at[:, mine_at], xa_s.at[u], xa_r.at[u], xpeer))
        if u < early:
            xb.append(remote(src.at[:, part_at], zb.at[:, part_at], xb_s.at[u], xb_r.at[u], xpeer))
        else:
            xb.append(remote(src.at[:, part_at], zpx.at[u], xb_s.at[u], xb_r.at[u], (pd, oh)))
    for u in range(early):
        xb[u].start()
        xa[u].start()

    grecv[0] = gpad[...]
    gcopies = [remote(gpad, grecv.at[o], gt_s.at[o], gt_r.at[o], (peer(o), t)) for o in range(1, n)]
    for copy in gcopies:
        copy.start()
    wcopy = pltpu.make_async_copy(w_hbm, w, w_sem)
    wcopy.start()
    tcopy = remote(attn_hbm, attn_p, t_s, t_r, partner)
    tcopy.start()
    gcopy.wait()

    def local_step(i, _):
        at = pl.ds(pl.multiple_of(i * tile, tile), tile)
        r = jnp.dot(three, g[:, at], preferred_element_type=F32)
        local[:, at] = r[:slots] + r[slots : 2 * slots] + r[2 * slots :]
        return 0

    lax.fori_loop(0, half // tile, local_step, 0)

    def slab(o):
        return pl.ds(pl.multiple_of(peer(o) * lw, lw), lw)

    lcopies = [
        remote(local.at[:, slab(o)], lrecv.at[o], l_s.at[o], l_r.at[o], (peer(o), t)) for o in range(1, n)
    ]
    for copy in lcopies:
        copy.start()
    lrecv[0] = local[:, slab(0)]

    def row_step(i, _):
        at = pl.ds(pl.multiple_of(i * tile, tile), tile)
        grow[:, at] = tdot(onehot[...], g[:, at])
        return 0

    lax.fori_loop(0, half // tile, row_step, 0)
    for copy in gcopies + lcopies:
        copy.wait_recv()

    def acopy(o, target):
        return remote(asend.at[o], arecv.at[o], a_s.at[o], a_r.at[o], (target, t))

    def sweep(i, carry):
        s = n - 1 - i
        slot = lax.rem(d - s + n, n)
        target = lax.rem(s - d + n, n)
        asend[target] = carry
        gates = grecv[slot]
        fresh = lrecv[slot]
        for k in range(slots):
            fresh = fresh + gates[:, k : k + 1] * carry[k : k + 1, :]

        @pl.when(target != 0)
        def _():
            acopy(target, s).start()

        return fresh

    lax.fori_loop(0, n, sweep, jnp.zeros((slots, lw), F32))
    acopies = [acopy(o, peer(o)) for o in range(1, n)]
    for o in range(n):
        if o:
            acopies[o - 1].wait_recv()
        src = lax.rem(d - o + n, n)
        at = pl.ds(pl.multiple_of(src * lw, lw), lw)
        got = arecv[o] if o else asend[0]
        after[:, at] = got
        rows[:, at] = (grow[:, at] + got).astype(BF16)
    rcopies = {}
    for u in range(early):
        for k, at in enumerate((cols(t, u, 1 - c), cols(t, u, c))):
            copy = remote(rows.at[:, at], rows_x.at[:, at], r_s.at[2 * u + k], r_r.at[2 * u + k], xpeer)
            copy.start()
            rcopies[u, k] = copy

    def fix(src, new_rows, dst, at):
        picked = jnp.dot(onehot[...], new_rows[:, at], preferred_element_type=F32)
        dst[:, at] = jnp.where(mask[...] > 0.5, picked, src[:, at].astype(F32)).astype(BF16)

    pcopies = [
        remote(za.at[:, cols(t, u, 1 - c)], zp.at[u], p_s.at[u], p_r.at[u], partner) for u in range(nu)
    ]
    qcopies = []
    for u in range(nu):
        if u < early:
            qcopies.append(remote(zb.at[:, cols(oh, u, 1 - c)], zpx.at[u], q_s.at[u], q_r.at[u], partner))
        else:
            qcopies.append(remote(zpx.at[u], zb.at[:, cols(oh, u, c)], q_s.at[u], q_r.at[u], partner))

    def fix_own(u):
        fix(g, rows, za, cols(t, u, 1 - c))
        fix(g, rows, za, cols(t, u, c))
        pcopies[u].start()
        if u >= early:

            @pl.when(c == 0)
            def _():
                xa[u].start()
                xb[u].start()

            @pl.when(c == 1)
            def _():
                xb[u].start()
                xa[u].start()

    for u in [*range(early, min(early + 2, nu)), *range(early), *range(early + 2, nu)]:
        fix_own(u)

    ycopies = {}

    def slot_of(own, u):
        return (0 if own else nu // 2) + u // 2

    def product(own, u, ht):
        zr, zq, at = (za, zp, cols(t, u, c)) if own else (zb, zpx, cols(oh, u, c))
        return tdot(zr[:, at], attn[:, ht]) + tdot(zq[u], attn_p[:, ht])

    def grad_block(own, u):
        slot = slot_of(own, u)

        def step(m, _):
            ht = pl.ds(pl.multiple_of(m * tile, tile), tile)
            r = product(own, u, ht)
            if is_other(u):
                ysend[slot, :, ht] = r.astype(BF16)
            else:
                kept[slot, :, ht] = r
            return 0

        lax.fori_loop(0, hd // tile, step, 0)
        if is_other(u):
            copy = remote(ysend.at[slot], yrecv.at[slot], y_s.at[slot], y_r.at[slot], ypeer)
            copy.start()
            ycopies[slot] = copy

    outer = (z == 0) | (z == nz - 1)
    low = z < zh
    inner_z = jnp.where(low, zh - 1, zh)

    def place(own, u):
        zd = zh * (t if own else oh) + level(t if own else oh, u // (2 * ns))
        across = (zd < zh) != low
        return slot_of(own, u), u % (2 * ns) // 2, zd, zd == z, across

    def at_chip(zt):
        return (zt * 4 + 2 * y + c, t)

    def to_relay(slot, ht, k):
        return remote(
            zsend.at[slot, :, ht], zpass.at[slot, :, ht], z_s.at[slot, k], v_r.at[slot, k], at_chip(inner_z)
        )

    def to_home(slot, piece, zd, k, ht, kind):
        return remote(
            zsend.at[slot, :, ht], zrecv.at[kind, piece, :, ht], z_s.at[slot, k], z_r.at[kind, piece], at_chip(zd)
        )

    def first_stage(own, u, total, ht, k):
        slot, piece, zd, at_home, across = place(own, u)

        @pl.when(at_home)
        def _():
            mine[piece, :, ht] = total

        @pl.when(across & jnp.logical_not(outer))
        def _():
            kept[slot, :, ht] = total

        @pl.when(across & outer)
        def _():
            zsend[slot, :, ht] = total.astype(BF16)
            to_relay(slot, ht, k).start()

        @pl.when(jnp.logical_not(across | at_home))
        def _():
            zsend[slot, :, ht] = total.astype(BF16)
            to_home(slot, piece, zd, k, ht, 1).start()

    def second_stage(own, u, ht, k):
        slot, piece, zd, _, across = place(own, u)

        @pl.when(across & jnp.logical_not(outer))
        def _():
            to_relay(slot, ht, k).wait_recv()
            zsend[slot, :, ht] = (kept[slot, :, ht] + zpass[slot, :, ht].astype(F32)).astype(BF16)
            to_home(slot, piece, zd, k, ht, 0).start()

    every = pl.ds(0, hd)

    def to_owner(own, u):
        slot = slot_of(own, u)
        ycopies[slot].wait_recv()
        first_stage(own, u, kept[slot] + yrecv[slot].astype(F32), every, 0)

    def last_block(u):
        slot = slot_of(False, u)
        ycopies[slot].wait_recv()
        for k in range(hd // tile):
            ht = pl.ds(k * tile, tile)
            first_stage(False, u, product(False, u, ht) + yrecv[slot, :, ht].astype(F32), ht, k)

    def pass_on(own, u):
        if not own and u == nu - 1:
            for k in range(hd // tile):
                second_stage(own, u, pl.ds(k * tile, tile), k)
        else:
            second_stage(own, u, every, 0)

    def own_attn():
        wcopy.wait()

        def step(m, _):
            at = pl.ds(pl.multiple_of(m * tile, tile), tile)
            k = pl.ds(pl.multiple_of(t * half, half), half)
            acc[:, at] = jnp.dot(za[...], w[k, at], preferred_element_type=F32)
            return 0

        lax.fori_loop(0, hd // tile, step, 0)

    def other_attn(r):
        from_at = wide(oh, r)
        last = r == zh - 1
        for u in range(2 * ns * r, 2 * ns * (r + 1)):
            if u >= early:
                qcopies[u].wait_recv()

        def step(m, _):
            at = pl.ds(pl.multiple_of(m * tile, tile), tile)
            k = pl.ds(pl.multiple_of(oh * half + from_at, 4 * bw), 4 * bw)
            total = acc[:, at] + jnp.dot(
                zb[:, pl.ds(from_at, 4 * bw)], w[k, at], preferred_element_type=F32
            )
            if last:
                out_attn[:, at] = total.astype(BF16)
            else:
                acc[:, at] = total
            return 0

        lax.fori_loop(0, hd // tile, step, 0)

    def memory():
        gates = gpad[...]

        def step(i, _):
            at = pl.ds(pl.multiple_of(i * tile, tile), tile)
            fresh = local[:, at]
            carry = after[:, at]
            for k in range(slots):
                fresh = fresh + gates[:, k : k + 1] * carry[k : k + 1, :]
            out_mem[:, at] = fresh
            return 0

        lax.fori_loop(0, half // tile, step, 0)

    waited = set()

    def once(name, copy):
        if name not in waited:
            waited.add(name)
            copy.wait_recv()

    attncopy.wait()
    for kind, u in plan(nu, ns, early):
        if kind == "own":
            once("attn", tcopy)
            pcopies[u].wait_recv()
            grad_block(True, u)
        elif kind == "prep":
            rcopies[u, 0].wait_recv()
            xb[u].wait_recv()
            fix(zb, rows_x, zb, cols(oh, u, 1 - c))
            qcopies[u].start()
            rcopies[u, 1].wait_recv()
            xa[u].wait_recv()
            fix(zb, rows_x, zb, cols(oh, u, c))
        elif kind == "other":
            if u < early:
                qcopies[u].wait_recv()
            else:
                xa[u].wait_recv()
                xb[u].wait_recv()
                qcopies[u].start()
            if u < nu - 1:
                grad_block(False, u)
            else:
                last_block(u)
        elif kind == "own_out":
            to_owner(True, u)
        elif kind in ("own_pass", "other_pass"):
            pass_on(kind == "own_pass", u)
        elif kind == "other_out":
            to_owner(False, u)
        elif kind == "own_attn":
            own_attn()
        elif kind == "attn":
            other_attn(u)
        else:
            memory()

    for piece in range(ns):
        total = mine[piece]
        for kind in range(2):
            to_home(0, piece, z, 0, every, kind).wait_recv()
            total = total + zrecv[kind, piece].astype(F32)
        out_w[pl.ds(piece * sub, sub), :] = total

    sent = xa + xb + gcopies + lcopies + acopies + pcopies + qcopies + list(ycopies.values())
    for copy in sent + [tcopy, *rcopies.values()]:
        copy.wait_send()
    for own in (True, False):
        for u in range(1, nu, 2):
            slot, _, _, at_home, _ = place(own, u)
            last = not own and u == nu - 1

            @pl.when(jnp.logical_not(at_home))
            def _(slot=slot, last=last):
                for k in range(hd // tile if last else 1):
                    to_relay(slot, pl.ds(k * tile, tile) if last else every, k).wait_send()


def settle(srcs, dsts, held, in_sem, out_sem):
    moves = []
    for src, dst, buf in zip(srcs, dsts, held):
        rows = min(128, src.shape[0])
        for i in range(src.shape[0] // rows):
            at = pl.ds(i * rows, rows)
            k = len(moves)
            moves.append(
                (
                    pltpu.make_async_copy(src.at[at], buf.at[at], in_sem.at[k]),
                    pltpu.make_async_copy(buf.at[at], dst.at[at], out_sem.at[k]),
                )
            )
    for fetch, _ in moves:
        fetch.start()
    for fetch, put in moves:
        fetch.wait()
        put.start()
    for _, put in moves:
        put.wait()


def settle_kernel(a, b, m, out_a, out_b, out_m, va, vb, vm, in_sem, out_sem):
    settle((a, b, m), (out_a, out_b, out_m), (va, vb, vm), in_sem, out_sem)


def settled(outs):
    shapes = [jax.ShapeDtypeStruct(o.shape, o.dtype) for o in outs]
    count = sum(o.shape[0] // min(128, o.shape[0]) for o in outs)
    return pl.pallas_call(
        settle_kernel,
        out_shape=tuple(shapes),
        in_specs=[pl.BlockSpec(memory_space=pl.ANY)] * 3,
        out_specs=tuple([pl.BlockSpec(memory_space=pl.ANY)] * 3),
        scratch_shapes=[pltpu.VMEM(o.shape, o.dtype) for o in outs]
        + [pltpu.SemaphoreType.DMA((count,)), pltpu.SemaphoreType.DMA((count,))],
    )(*outs)


def fused(n, attn_out, out_proj_t, grad_out, read_weights, memory_gate, write_pos):
    seg, half = grad_out.shape
    hd = attn_out.shape[1]
    slots = write_pos.shape[1]
    depth = out_proj_t.shape[0]
    bw, lw, nz = depth // n, half // n, n // 4
    sub = 128
    ns = bw // sub
    nu = nz * ns
    early = EARLY
    V = pltpu.VMEM
    D = pltpu.SemaphoreType.DMA
    vmem = pl.BlockSpec(memory_space=pltpu.VMEM)
    outs = pl.pallas_call(
        functools.partial(kernel, n, early),
        out_shape=(
            jax.ShapeDtypeStruct((seg, hd), BF16),
            jax.ShapeDtypeStruct((bw, hd), F32),
            jax.ShapeDtypeStruct((slots, half), F32),
        ),
        in_specs=[pl.BlockSpec(memory_space=pl.ANY)] * 6,
        out_specs=(vmem, vmem, vmem),
        scratch_shapes=[
            V((slots, seg), F32),
            V((slots, slots), F32),
            V((1, slots), jnp.int32),
            V((seg, half), BF16),
            V((seg, hd), BF16),
            V((depth, hd), BF16),
            V((seg, hd), BF16),
            V((seg, half), BF16),
            V((seg, half), BF16),
            V((nu, seg, sub), BF16),
            V((nu, seg, sub), BF16),
            V((seg, hd), F32),
            V((seg, slots), BF16),
            V((seg, sub), F32),
            V((slots, half), F32),
            V((slots, half), BF16),
            V((slots, half), BF16),
            V((slots, half), F32),
            V((slots, half), F32),
            V((slots, 128), F32),
            V((n, slots, 128), F32),
            V((n, slots, lw), F32),
            V((n, slots, lw), F32),
            V((n, slots, lw), F32),
            V((nu, sub, hd), BF16),
            V((nu, sub, hd), BF16),
            V((nu, sub, hd), F32),
            V((nu, sub, hd), BF16),
            V((nu, sub, hd), BF16),
            V((2, ns, sub, hd), BF16),
            V((ns, sub, hd), F32),
            D((3,)),
            D,
            D,
            D,
            D((nu,)),
            D((nu,)),
            D((nu,)),
            D((nu,)),
            D((n,)),
            D((n,)),
            D((n,)),
            D((n,)),
            D((n,)),
            D((n,)),
            D((2 * early,)),
            D((2 * early,)),
            D,
            D,
            D((nu,)),
            D((nu,)),
            D((nu,)),
            D((nu,)),
            D((nu,)),
            D((nu,)),
            D((nu, hd // 256)),
            D((nu, hd // 256)),
            D((2, ns)),
        ],
        compiler_params=pltpu.CompilerParams(
            collective_id=0, has_side_effects=True, vmem_limit_bytes=62 * 1024 * 1024
        ),
    )(attn_out, out_proj_t, grad_out, read_weights.T, memory_gate, write_pos)
    return settled(outs)


def plain(attn_out, out_proj_t, grad_out, read_weights, memory_gate, write_pos):
    high = lax.Precision.HIGHEST
    seg_len = attn_out.shape[0]
    slots = write_pos.shape[1]
    gate_at_step = memory_gate.T
    dy_cols = grad_out.astype(jnp.float32)
    local = jnp.dot(read_weights.T, dy_cols, precision=high, preferred_element_type=jnp.float32)
    all_gates, all_terms = (
        lax.all_gather(gate_at_step, "dp", axis=0, tiled=True),
        lax.all_gather(local, "dp", axis=0, tiled=True),
    )
    count = lax.axis_size("dp")
    mine = lax.axis_index("dp")

    def sweep(step, carry):
        which = (count - 1 - step).astype(jnp.int32)
        gate = lax.dynamic_slice_in_dim(all_gates, which * slots, slots, 0)
        term = lax.dynamic_slice_in_dim(all_terms, which * slots, slots, 0)
        fresh = jnp.dot(gate, carry, precision=high, preferred_element_type=jnp.float32) + term
        return jnp.where(which > mine, fresh, carry)

    after = lax.fori_loop(0, count, sweep, jnp.zeros_like(local))
    grad_memory = (
        jnp.dot(gate_at_step, after, precision=high, preferred_element_type=jnp.float32) + local
    )
    places = jnp.arange(seg_len, dtype=jnp.int32)
    onehot = (places[:, None] == write_pos[0][None, :]).astype(jnp.float32)
    written = jnp.dot(onehot, after, precision=high, preferred_element_type=jnp.float32)
    grad_z = (dy_cols + written).astype(jnp.bfloat16)
    full_z = lax.all_gather(grad_z, "tensor", axis=1, tiled=True)
    grad_attn = jnp.dot(full_z, out_proj_t, preferred_element_type=jnp.float32).astype(jnp.bfloat16)
    term = lax.dot_general(
        full_z, attn_out, (((0,), (0,)), ((), ())), preferred_element_type=jnp.float32
    )
    grad_weight = lax.psum_scatter(term, "dp", scatter_dimension=0, tiled=True)
    return (grad_attn, grad_weight, grad_memory)


def solution(mesh):
    n = mesh.shape["dp"]
    parts = mesh.shape["tensor"]

    def body(attn_out, out_proj_t, grad_out, read_weights, memory_gate, write_pos):
        half, hd = grad_out.shape[1], attn_out.shape[1]
        fits = (
            parts == 2
            and n // 4 == 4
            and half % (n * 128) == 0
            and half % 256 == 0
            and hd % 256 == 0
            and out_proj_t.shape[0] <= 4096
        )
        args = (attn_out, out_proj_t, grad_out, read_weights, memory_gate, write_pos)
        return fused(n, *args) if fits else plain(*args)

    return jax.shard_map(
        body,
        mesh=mesh,
        in_specs=(
            P("dp", "tensor"),
            P(None, "tensor"),
            P("dp", "tensor"),
            P("dp", None),
            P("dp", None),
            P("dp", None),
        ),
        out_specs=(P("dp", "tensor"), P("dp", "tensor"), P("dp", "tensor")),
        check_vma=False,
    )
```

```python
import functools

import jax
import jax.numpy as jnp
from jax import lax
from jax.experimental import pallas as pl
from jax.experimental.pallas import tpu as pltpu
from jax.sharding import PartitionSpec as P

MESH = pl.DeviceIdType.MESH
F32 = jnp.float32
BF16 = jnp.bfloat16
EARLY = 2


def split3(a):
    hi = a.astype(BF16)
    rest = a - hi.astype(F32)
    mid = rest.astype(BF16)
    low = (rest - mid.astype(F32)).astype(BF16)
    return jnp.concatenate([hi, mid, low], axis=0)


def tdot(a, b):
    return lax.dot_general(a, b, (((0,), (0,)), ((), ())), preferred_element_type=F32)


def plan(nu, ns, early):
    steps = []
    for u in range(nu):
        lead = u < nu // 2
        own = 2.0 + 0.2 * u if lead else (3.05 + 0.05 * (u - nu // 2) if u < nu - 2 else 5.15 + 0.05 * (u + 2 - nu))
        steps.append((own, "own", u))
        if u < early:
            steps.append((early + 0.1 + 0.25 * u, "prep", u))
            arrived = early + 0.2 + 0.25 * u
        else:
            arrived = u + 1.0
        steps.append((arrived, "other", u))
        if u % 2:
            sent = max(own + 0.01, 3.05 + 0.67 * (u - 1))
            steps.append((sent, "own_out", u))
            steps.append((sent + 0.9, "own_pass", u))
            sent = max(arrived + 0.01, 3.7 + 0.66 * (u - 1))
            if u < nu - 1:
                steps.append((sent, "other_out", u))
            steps.append((sent + (0.9 if u < nu - 1 else 0.1), "other_pass", u))
        if (u + 1) % (2 * ns) == 0 and u < nu - 1:
            steps.append((arrived + 1.5, "attn", u // (2 * ns)))
        if u == nu - 2:
            steps.append((arrived + 0.2, "attn_part", range(nu - 2 * ns, nu - 1)))
        if u == nu - 1:
            steps.append((arrived + 1.0, "attn_part", range(u, nu)))
    steps.append((4.2, "own_attn", 0))
    steps.append((4.25, "memory", 0))
    return [step[1:] for step in sorted(steps, key=lambda step: step[0])]


def kernel(
    n, early, attn_hbm, w_hbm, g_hbm, rwt_hbm, gate_hbm, wpos_hbm, out_attn, out_w, out_mem,
    rwt, gate, wpos, g, attn, w, attn_p, za, zb, zp, zpx, acc, onehot, mask, grow, rows, rows_x, local, after,
    gpad, grecv, lrecv, asend, arecv, ysend, yrecv, kept, zsend, zpass, zrecv, mine,
    small_sem, g_sem, attn_sem, w_sem, xa_s, xa_r, xb_s, xb_r, gt_s, gt_r, l_s, l_r, a_s, a_r, r_s, r_r, t_s, t_r,
    p_s, p_r, q_s, q_r, y_s, y_r, z_s, v_r, z_r,
):
    d = lax.axis_index("dp")
    t = lax.axis_index("tensor")
    c = lax.rem(d, 2)
    y = lax.rem(d // 2, 2)
    z = d // 4
    nz = n // 4
    seg, half = g.shape
    hd = attn.shape[1]
    slots = rwt.shape[0]
    bw = 2 * half // n
    lw = half // n
    zh = nz // 2
    sub = mask.shape[1]
    ns = bw // sub
    nu = 2 * zh * ns
    oh = 1 - t
    pd = d + 1 - 2 * c
    partner = (pd, t)
    xpeer = (d, oh)
    ypeer = (d + 2 - 4 * y, t)
    tile = 256

    def remote(src, dst, ss, rs, dev):
        return pltpu.make_async_remote_copy(
            src_ref=src, dst_ref=dst, send_sem=ss, recv_sem=rs, device_id=dev, device_id_type=MESH
        )

    def peer(o):
        return lax.rem(d + o, n)

    barrier = pltpu.get_barrier_semaphore()
    for o in range(1, n):
        pl.semaphore_signal(barrier, inc=1, device_id=(peer(o), t), device_id_type=MESH)
    pl.semaphore_signal(barrier, inc=1, device_id=xpeer, device_id_type=MESH)
    pl.semaphore_signal(barrier, inc=1, device_id=(pd, oh), device_id_type=MESH)

    smalls = [
        pltpu.make_async_copy(src, dst, small_sem.at[i])
        for i, (src, dst) in enumerate(((rwt_hbm, rwt), (gate_hbm, gate), (wpos_hbm, wpos)))
    ]
    for copy in smalls:
        copy.start()
    gcopy = pltpu.make_async_copy(g_hbm, g, g_sem)
    gcopy.start()
    attncopy = pltpu.make_async_copy(attn_hbm, attn, attn_sem)
    attncopy.start()
    pl.semaphore_wait(barrier, n + 1)

    def is_other(u):
        return u % 2 == 0

    def level(h, r):
        return r + h * (zh - 1 - 2 * r)

    def cols(h, u, par):
        yd = 1 - y if is_other(u) else y
        j = 2 * level(h, u // (2 * ns)) + yd
        piece = u % (2 * ns) // 2
        return pl.ds(pl.multiple_of((2 * j + par) * bw + piece * sub, sub), sub)

    def wide(h, r):
        return pl.multiple_of(4 * level(h, r) * bw, 4 * bw)

    xa, xb = [], []
    for u in range(nu):
        mine_at, part_at = cols(t, u, c), cols(t, u, 1 - c)
        src = g_hbm if u < early else za
        xa.append(remote(src.at[:, mine_at], zb.at[:, mine_at], xa_s.at[u], xa_r.at[u], xpeer))
        if u < early:
            xb.append(remote(src.at[:, part_at], zb.at[:, part_at], xb_s.at[u], xb_r.at[u], xpeer))
        else:
            xb.append(remote(src.at[:, part_at], zpx.at[u], xb_s.at[u], xb_r.at[u], (pd, oh)))
    for u in range(early):
        xb[u].start()
        xa[u].start()

    for copy in smalls:
        copy.wait()
    gpad[...] = jnp.zeros_like(gpad)
    gpad[:, :slots] = gate[...].T
    grecv[0] = gpad[...]
    gcopies = [remote(gpad, grecv.at[o], gt_s.at[o], gt_r.at[o], (peer(o), t)) for o in range(1, n)]
    for copy in gcopies:
        copy.start()
    wcopy = pltpu.make_async_copy(w_hbm, w, w_sem)
    wcopy.start()
    tcopy = remote(attn_hbm, attn_p, t_s, t_r, partner)
    tcopy.start()
    three = split3(rwt[...])
    gcopy.wait()

    def local_step(i, _):
        at = pl.ds(pl.multiple_of(i * tile, tile), tile)
        r = jnp.dot(three, g[:, at], preferred_element_type=F32)
        local[:, at] = r[:slots] + r[slots : 2 * slots] + r[2 * slots :]
        return 0

    lax.fori_loop(0, half // tile, local_step, 0)

    def slab(o):
        return pl.ds(pl.multiple_of(peer(o) * lw, lw), lw)

    lcopies = [
        remote(local.at[:, slab(o)], lrecv.at[o], l_s.at[o], l_r.at[o], (peer(o), t)) for o in range(1, n)
    ]
    for copy in lcopies:
        copy.start()
    lrecv[0] = local[:, slab(0)]

    place_of = lax.broadcasted_iota(jnp.int32, (seg, slots), 0)
    hit = jnp.where(place_of == wpos[...], 1.0, 0.0)
    onehot[...] = hit.astype(BF16)
    mask[...] = jnp.broadcast_to(jnp.sum(hit, axis=1, keepdims=True), mask.shape)

    def row_step(i, _):
        at = pl.ds(pl.multiple_of(i * tile, tile), tile)
        grow[:, at] = tdot(onehot[...], g[:, at])
        return 0

    lax.fori_loop(0, half // tile, row_step, 0)
    for copy in gcopies + lcopies:
        copy.wait_recv()

    def acopy(o, target):
        return remote(asend.at[o], arecv.at[o], a_s.at[o], a_r.at[o], (target, t))

    def sweep(i, carry):
        s = n - 1 - i
        slot = lax.rem(d - s + n, n)
        target = lax.rem(s - d + n, n)
        asend[target] = carry
        gates = grecv[slot]
        fresh = lrecv[slot]
        for k in range(slots):
            fresh = fresh + gates[:, k : k + 1] * carry[k : k + 1, :]

        @pl.when(target != 0)
        def _():
            acopy(target, s).start()

        return fresh

    lax.fori_loop(0, n, sweep, jnp.zeros((slots, lw), F32))
    acopies = [acopy(o, peer(o)) for o in range(1, n)]
    for o in range(n):
        if o:
            acopies[o - 1].wait_recv()
        src = lax.rem(d - o + n, n)
        at = pl.ds(pl.multiple_of(src * lw, lw), lw)
        got = arecv[o] if o else asend[0]
        after[:, at] = got
        rows[:, at] = (grow[:, at] + got).astype(BF16)
    rcopies = {}
    for u in range(early):
        for k, at in enumerate((cols(t, u, 1 - c), cols(t, u, c))):
            copy = remote(rows.at[:, at], rows_x.at[:, at], r_s.at[2 * u + k], r_r.at[2 * u + k], xpeer)
            copy.start()
            rcopies[u, k] = copy

    def fix(src, new_rows, dst, at):
        picked = jnp.dot(onehot[...], new_rows[:, at], preferred_element_type=F32)
        dst[:, at] = jnp.where(mask[...] > 0.5, picked, src[:, at].astype(F32)).astype(BF16)

    pcopies = [
        remote(za.at[:, cols(t, u, 1 - c)], zp.at[u], p_s.at[u], p_r.at[u], partner) for u in range(nu)
    ]
    qcopies = []
    for u in range(nu):
        if u < early:
            qcopies.append(remote(zb.at[:, cols(oh, u, 1 - c)], zpx.at[u], q_s.at[u], q_r.at[u], partner))
        else:
            qcopies.append(remote(zpx.at[u], zb.at[:, cols(oh, u, c)], q_s.at[u], q_r.at[u], partner))

    def fix_own(u):
        fix(g, rows, za, cols(t, u, 1 - c))
        fix(g, rows, za, cols(t, u, c))
        pcopies[u].start()
        if u >= early:

            @pl.when(c == 0)
            def _():
                xa[u].start()
                xb[u].start()

            @pl.when(c == 1)
            def _():
                xb[u].start()
                xa[u].start()

    for u in [*range(early, min(early + 2, nu)), *range(early), *range(early + 2, nu)]:
        fix_own(u)

    ycopies = {}

    def slot_of(own, u):
        return (0 if own else nu // 2) + u // 2

    def product(own, u, ht):
        zr, zq, at = (za, zp, cols(t, u, c)) if own else (zb, zpx, cols(oh, u, c))
        return tdot(zr[:, at], attn[:, ht]) + tdot(zq[u], attn_p[:, ht])

    def grad_block(own, u):
        slot = slot_of(own, u)

        def step(m, _):
            ht = pl.ds(pl.multiple_of(m * tile, tile), tile)
            r = product(own, u, ht)
            if is_other(u):
                ysend[slot, :, ht] = r.astype(BF16)
            else:
                kept[slot, :, ht] = r
            return 0

        lax.fori_loop(0, hd // tile, step, 0)
        if is_other(u):
            copy = remote(ysend.at[slot], yrecv.at[slot], y_s.at[slot], y_r.at[slot], ypeer)
            copy.start()
            ycopies[slot] = copy

    outer = (z == 0) | (z == nz - 1)
    low = z < zh
    inner_z = jnp.where(low, zh - 1, zh)

    def place(own, u):
        zd = zh * (t if own else oh) + level(t if own else oh, u // (2 * ns))
        across = (zd < zh) != low
        return slot_of(own, u), u % (2 * ns) // 2, zd, zd == z, across

    def at_chip(zt):
        return (zt * 4 + 2 * y + c, t)

    def to_relay(slot, ht, k):
        return remote(
            zsend.at[slot, :, ht], zpass.at[slot, :, ht], z_s.at[slot, k], v_r.at[slot, k], at_chip(inner_z)
        )

    def to_home(slot, piece, zd, k, ht, kind):
        return remote(
            zsend.at[slot, :, ht], zrecv.at[kind, piece, :, ht], z_s.at[slot, k], z_r.at[kind, piece], at_chip(zd)
        )

    def first_stage(own, u, total, ht, k):
        slot, piece, zd, at_home, across = place(own, u)

        @pl.when(at_home)
        def _():
            mine[piece, :, ht] = total

        @pl.when(across & jnp.logical_not(outer))
        def _():
            kept[slot, :, ht] = total

        @pl.when(across & outer)
        def _():
            zsend[slot, :, ht] = total.astype(BF16)
            to_relay(slot, ht, k).start()

        @pl.when(jnp.logical_not(across | at_home))
        def _():
            zsend[slot, :, ht] = total.astype(BF16)
            to_home(slot, piece, zd, k, ht, 1).start()

    def second_stage(own, u, ht, k):
        slot, piece, zd, _, across = place(own, u)

        @pl.when(across & jnp.logical_not(outer))
        def _():
            to_relay(slot, ht, k).wait_recv()
            zsend[slot, :, ht] = (kept[slot, :, ht] + zpass[slot, :, ht].astype(F32)).astype(BF16)
            to_home(slot, piece, zd, k, ht, 0).start()

    every = pl.ds(0, hd)

    def to_owner(own, u):
        slot = slot_of(own, u)
        ycopies[slot].wait_recv()
        first_stage(own, u, kept[slot] + yrecv[slot].astype(F32), every, 0)

    def last_block(u):
        slot = slot_of(False, u)
        ycopies[slot].wait_recv()
        for k in range(hd // tile):
            ht = pl.ds(k * tile, tile)
            first_stage(False, u, product(False, u, ht) + yrecv[slot, :, ht].astype(F32), ht, k)

    def pass_on(own, u):
        if not own and u == nu - 1:
            for k in range(hd // tile):
                second_stage(own, u, pl.ds(k * tile, tile), k)
        else:
            second_stage(own, u, every, 0)

    def own_attn():
        wcopy.wait()

        def step(m, _):
            at = pl.ds(pl.multiple_of(m * tile, tile), tile)
            k = pl.ds(pl.multiple_of(t * half, half), half)
            acc[:, at] = jnp.dot(za[...], w[k, at], preferred_element_type=F32)
            return 0

        lax.fori_loop(0, hd // tile, step, 0)

    def other_attn(r):
        from_at = wide(oh, r)
        for u in range(2 * ns * r, 2 * ns * (r + 1)):
            if u >= early:
                qcopies[u].wait_recv()

        def step(m, _):
            at = pl.ds(pl.multiple_of(m * tile, tile), tile)
            k = pl.ds(pl.multiple_of(oh * half + from_at, 4 * bw), 4 * bw)
            total = acc[:, at] + jnp.dot(
                zb[:, pl.ds(from_at, 4 * bw)], w[k, at], preferred_element_type=F32
            )
            acc[:, at] = total
            return 0

        lax.fori_loop(0, hd // tile, step, 0)

    def part_attn(units):
        for u in units:
            if u >= early:
                qcopies[u].wait_recv()
        places = [cols(oh, u, par) for u in units for par in range(2)]

        def step(m, _):
            at = pl.ds(pl.multiple_of(m * tile, tile), tile)
            lhs = jnp.concatenate([zb[:, k] for k in places], axis=1)
            rhs = jnp.concatenate(
                [w[pl.ds(pl.multiple_of(oh * half + k.start, sub), sub), at] for k in places], axis=0
            )
            total = acc[:, at] + jnp.dot(lhs, rhs, preferred_element_type=F32)
            if nu - 1 in units:
                out_attn[:, at] = total.astype(BF16)
            else:
                acc[:, at] = total
            return 0

        lax.fori_loop(0, hd // tile, step, 0)

    def memory():
        gates = gpad[...]

        def step(i, _):
            at = pl.ds(pl.multiple_of(i * tile, tile), tile)
            fresh = local[:, at]
            carry = after[:, at]
            for k in range(slots):
                fresh = fresh + gates[:, k : k + 1] * carry[k : k + 1, :]
            out_mem[:, at] = fresh
            return 0

        lax.fori_loop(0, half // tile, step, 0)

    waited = set()

    def once(name, copy):
        if name not in waited:
            waited.add(name)
            copy.wait_recv()

    attncopy.wait()
    for kind, u in plan(nu, ns, early):
        if kind == "own":
            once("attn", tcopy)
            pcopies[u].wait_recv()
            grad_block(True, u)
        elif kind == "prep":
            rcopies[u, 0].wait_recv()
            xb[u].wait_recv()
            fix(zb, rows_x, zb, cols(oh, u, 1 - c))
            qcopies[u].start()
            rcopies[u, 1].wait_recv()
            xa[u].wait_recv()
            fix(zb, rows_x, zb, cols(oh, u, c))
        elif kind == "other":
            if u < early:
                qcopies[u].wait_recv()
            else:
                xa[u].wait_recv()
                xb[u].wait_recv()
                qcopies[u].start()
            if u < nu - 1:
                grad_block(False, u)
            else:
                last_block(u)
        elif kind == "own_out":
            to_owner(True, u)
        elif kind in ("own_pass", "other_pass"):
            pass_on(kind == "own_pass", u)
        elif kind == "other_out":
            to_owner(False, u)
        elif kind == "own_attn":
            own_attn()
        elif kind == "attn":
            other_attn(u)
        elif kind == "attn_part":
            part_attn(u)
        else:
            memory()

    for piece in range(ns):
        total = mine[piece]
        for kind in range(2):
            to_home(0, piece, z, 0, every, kind).wait_recv()
            total = total + zrecv[kind, piece].astype(F32)
        out_w[pl.ds(piece * sub, sub), :] = total

    sent = xa + xb + gcopies + lcopies + acopies + pcopies + qcopies + list(ycopies.values())
    for copy in sent + [tcopy, *rcopies.values()]:
        copy.wait_send()
    for own in (True, False):
        for u in range(1, nu, 2):
            slot, _, _, at_home, _ = place(own, u)
            last = not own and u == nu - 1

            @pl.when(jnp.logical_not(at_home))
            def _(slot=slot, last=last):
                for k in range(hd // tile if last else 1):
                    to_relay(slot, pl.ds(k * tile, tile) if last else every, k).wait_send()


def settle_kernel(a, b, m, out_a, out_b, out_m, sems):
    copies = [
        pltpu.make_async_copy(src, dst, sems.at[i])
        for i, (src, dst) in enumerate(((a, out_a), (b, out_b), (m, out_m)))
    ]
    for copy in copies:
        copy.start()
    for copy in copies:
        copy.wait()


def settled(outs):
    return pl.pallas_call(
        settle_kernel,
        out_shape=tuple(jax.ShapeDtypeStruct(o.shape, o.dtype) for o in outs),
        in_specs=[pl.BlockSpec(memory_space=pltpu.VMEM)] * 3,
        out_specs=tuple([pl.BlockSpec(memory_space=pl.ANY)] * 3),
        scratch_shapes=[pltpu.SemaphoreType.DMA((3,))],
    )(*[pltpu.with_memory_space_constraint(o, pltpu.VMEM) for o in outs])


def fused(n, attn_out, out_proj_t, grad_out, read_weights, memory_gate, write_pos):
    seg, half = grad_out.shape
    hd = attn_out.shape[1]
    slots = write_pos.shape[1]
    depth = out_proj_t.shape[0]
    bw, lw, nz = depth // n, half // n, n // 4
    sub = 128
    ns = bw // sub
    nu = nz * ns
    early = EARLY
    V = pltpu.VMEM
    D = pltpu.SemaphoreType.DMA
    vmem = pl.BlockSpec(memory_space=pltpu.VMEM)
    outs = pl.pallas_call(
        functools.partial(kernel, n, early),
        out_shape=(V((seg, hd), BF16), V((bw, hd), F32), V((slots, half), F32)),
        in_specs=[pl.BlockSpec(memory_space=pl.ANY)] * 6,
        out_specs=(vmem, vmem, vmem),
        scratch_shapes=[
            V((slots, seg), F32),
            V((slots, slots), F32),
            V((1, slots), jnp.int32),
            V((seg, half), BF16),
            V((seg, hd), BF16),
            V((depth, hd), BF16),
            V((seg, hd), BF16),
            V((seg, half), BF16),
            V((seg, half), BF16),
            V((nu, seg, sub), BF16),
            V((nu, seg, sub), BF16),
            V((seg, hd), F32),
            V((seg, slots), BF16),
            V((seg, sub), F32),
            V((slots, half), F32),
            V((slots, half), BF16),
            V((slots, half), BF16),
            V((slots, half), F32),
            V((slots, half), F32),
            V((slots, 128), F32),
            V((n, slots, 128), F32),
            V((n, slots, lw), F32),
            V((n, slots, lw), F32),
            V((n, slots, lw), F32),
            V((nu, sub, hd), BF16),
            V((nu, sub, hd), BF16),
            V((nu, sub, hd), F32),
            V((nu, sub, hd), BF16),
            V((nu, sub, hd), BF16),
            V((2, ns, sub, hd), BF16),
            V((ns, sub, hd), F32),
            D((3,)),
            D,
            D,
            D,
            D((nu,)),
            D((nu,)),
            D((nu,)),
            D((nu,)),
            D((n,)),
            D((n,)),
            D((n,)),
            D((n,)),
            D((n,)),
            D((n,)),
            D((2 * early,)),
            D((2 * early,)),
            D,
            D,
            D((nu,)),
            D((nu,)),
            D((nu,)),
            D((nu,)),
            D((nu,)),
            D((nu,)),
            D((nu, hd // 256)),
            D((nu, hd // 256)),
            D((2, ns)),
        ],
        compiler_params=pltpu.CompilerParams(
            collective_id=0, has_side_effects=True, vmem_limit_bytes=52 * 1024 * 1024
        ),
    )(attn_out, out_proj_t, grad_out, read_weights.T, memory_gate, write_pos)
    return settled(outs)


def plain(attn_out, out_proj_t, grad_out, read_weights, memory_gate, write_pos):
    high = lax.Precision.HIGHEST
    seg_len = attn_out.shape[0]
    slots = write_pos.shape[1]
    gate_at_step = memory_gate.T
    dy_cols = grad_out.astype(jnp.float32)
    local = jnp.dot(read_weights.T, dy_cols, precision=high, preferred_element_type=jnp.float32)
    all_gates, all_terms = (
        lax.all_gather(gate_at_step, "dp", axis=0, tiled=True),
        lax.all_gather(local, "dp", axis=0, tiled=True),
    )
    count = lax.axis_size("dp")
    mine = lax.axis_index("dp")

    def sweep(step, carry):
        which = (count - 1 - step).astype(jnp.int32)
        gate = lax.dynamic_slice_in_dim(all_gates, which * slots, slots, 0)
        term = lax.dynamic_slice_in_dim(all_terms, which * slots, slots, 0)
        fresh = jnp.dot(gate, carry, precision=high, preferred_element_type=jnp.float32) + term
        return jnp.where(which > mine, fresh, carry)

    after = lax.fori_loop(0, count, sweep, jnp.zeros_like(local))
    grad_memory = (
        jnp.dot(gate_at_step, after, precision=high, preferred_element_type=jnp.float32) + local
    )
    places = jnp.arange(seg_len, dtype=jnp.int32)
    onehot = (places[:, None] == write_pos[0][None, :]).astype(jnp.float32)
    written = jnp.dot(onehot, after, precision=high, preferred_element_type=jnp.float32)
    grad_z = (dy_cols + written).astype(jnp.bfloat16)
    full_z = lax.all_gather(grad_z, "tensor", axis=1, tiled=True)
    grad_attn = jnp.dot(full_z, out_proj_t, preferred_element_type=jnp.float32).astype(jnp.bfloat16)
    term = lax.dot_general(
        full_z, attn_out, (((0,), (0,)), ((), ())), preferred_element_type=jnp.float32
    )
    grad_weight = lax.psum_scatter(term, "dp", scatter_dimension=0, tiled=True)
    return (grad_attn, grad_weight, grad_memory)


def solution(mesh):
    n = mesh.shape["dp"]
    parts = mesh.shape["tensor"]

    def body(attn_out, out_proj_t, grad_out, read_weights, memory_gate, write_pos):
        half, hd = grad_out.shape[1], attn_out.shape[1]
        fits = (
            parts == 2
            and n // 4 == 4
            and half % (n * 128) == 0
            and half % 256 == 0
            and hd % 256 == 0
            and out_proj_t.shape[0] <= 4096
        )
        args = (attn_out, out_proj_t, grad_out, read_weights, memory_gate, write_pos)
        return fused(n, *args) if fits else plain(*args)

    return jax.shard_map(
        body,
        mesh=mesh,
        in_specs=(
            P("dp", "tensor"),
            P(None, "tensor"),
            P("dp", "tensor"),
            P("dp", None),
            P("dp", None),
            P("dp", None),
        ),
        out_specs=(P("dp", "tensor"), P("dp", "tensor"), P("dp", "tensor")),
        check_vma=False,
    )
```

```python
import functools

import jax
import jax.numpy as jnp
from jax import lax
from jax.experimental import pallas as pl
from jax.experimental.pallas import tpu as pltpu
from jax.sharding import PartitionSpec as P

MESH = pl.DeviceIdType.MESH
F32 = jnp.float32
BF16 = jnp.bfloat16
EARLY = 2


def split3(a):
    hi = a.astype(BF16)
    rest = a - hi.astype(F32)
    mid = rest.astype(BF16)
    low = (rest - mid.astype(F32)).astype(BF16)
    return jnp.concatenate([hi, mid, low], axis=0)


def tdot(a, b):
    return lax.dot_general(a, b, (((0,), (0,)), ((), ())), preferred_element_type=F32)


def plan(nu, ns, early):
    steps = []
    for u in range(nu):
        lead = u < nu // 2
        own = 2.0 + 0.2 * u if lead else (3.05 + 0.05 * (u - nu // 2) if u < nu - 2 else 5.15 + 0.05 * (u + 2 - nu))
        steps.append((own, "own", u))
        if u < early:
            steps.append((early + 0.1 + 0.25 * u, "prep", u))
            arrived = early + 0.2 + 0.25 * u
        else:
            arrived = u + 1.0
        steps.append((arrived, "other", u))
        if u % 2:
            sent = max(own + 0.01, 3.05 + 0.67 * (u - 1))
            steps.append((sent, "own_out", u))
            steps.append((sent + 1.3, "own_pass", u))
            sent = max(arrived + 0.01, 3.7 + 0.66 * (u - 1))
            if u < nu - 1:
                steps.append((sent, "other_out", u))
            steps.append((sent + (1.2 if u < nu - 1 else 0.1), "other_pass", u))
        if (u + 1) % (2 * ns) == 0 and u < nu - 1:
            steps.append((arrived + 1.5, "attn", u // (2 * ns)))
        if u == nu - 2:
            steps.append((arrived + 0.2, "attn_part1", range(nu - 2 * ns, nu - 1)))
        if u == nu - 1:
            steps.append((arrived + 1.0, "attn_part0", range(nu - 2 * ns, nu - 1)))
            steps.append((arrived + 1.1, "attn_part", range(u, nu)))
    steps.append((4.2, "own_attn", 0))
    steps.append((4.25, "memory", 0))
    return [step[1:] for step in sorted(steps, key=lambda step: step[0])]


def kernel(
    n, early, attn_hbm, w_hbm, g_hbm, rwt_hbm, gate_hbm, wpos_hbm, out_attn, out_w, out_mem,
    rwt, gate, wpos, g, attn, w, attn_p, za, zb, zp, zpx, acc, onehot, mask, grow, rows, rows_x, local, after,
    gpad, grecv, lrecv, asend, arecv, ysend, yrecv, kept, zsend, zpass, zrecv, mine,
    small_sem, g_sem, attn_sem, w_sem, x_s, x_r, gt_s, gt_r, l_s, l_r, a_s, a_r, r_s, r_r, t_s, t_r,
    p_s, p_r, q_s, q_r, y_s, y_r, z_s, v_r, z_r,
):
    d = lax.axis_index("dp")
    t = lax.axis_index("tensor")
    c = lax.rem(d, 2)
    y = lax.rem(d // 2, 2)
    z = d // 4
    nz = n // 4
    seg, half = g.shape
    hd = attn.shape[1]
    slots = rwt.shape[0]
    bw = 2 * half // n
    lw = half // n
    zh = nz // 2
    sub = mask.shape[1]
    ns = bw // sub
    nu = 2 * zh * ns
    oh = 1 - t
    pd = d + 1 - 2 * c
    partner = (pd, t)
    xpeer = (d, oh)
    ypeer = (d + 2 - 4 * y, t)
    tile = 256

    def remote(src, dst, ss, rs, dev):
        return pltpu.make_async_remote_copy(
            src_ref=src, dst_ref=dst, send_sem=ss, recv_sem=rs, device_id=dev, device_id_type=MESH
        )

    def all_sent(ref, sem):
        remote(ref, ref, sem, sem, xpeer).wait_send()

    def all_here(ref, sem):
        remote(ref, ref, sem, sem, xpeer).wait_recv()

    def peer(o):
        return lax.rem(d + o, n)

    barrier = pltpu.get_barrier_semaphore()
    for o in range(1, n):
        pl.semaphore_signal(barrier, inc=1, device_id=(peer(o), t), device_id_type=MESH)
    pl.semaphore_signal(barrier, inc=1, device_id=xpeer, device_id_type=MESH)
    pl.semaphore_signal(barrier, inc=1, device_id=(pd, oh), device_id_type=MESH)

    smalls = [
        pltpu.make_async_copy(src, dst, small_sem.at[i])
        for i, (src, dst) in enumerate(((rwt_hbm, rwt), (gate_hbm, gate), (wpos_hbm, wpos)))
    ]
    for copy in smalls:
        copy.start()
    gcopy = pltpu.make_async_copy(g_hbm, g, g_sem)
    gcopy.start()
    attncopy = pltpu.make_async_copy(attn_hbm, attn, attn_sem)
    attncopy.start()
    pl.semaphore_wait(barrier, n + 1)

    def is_other(u):
        return u % 2 == 0

    def level(h, r):
        return r + h * (zh - 1 - 2 * r)

    def cols(h, u, par):
        yd = 1 - y if is_other(u) else y
        j = 2 * level(h, u // (2 * ns)) + yd
        piece = u % (2 * ns) // 2
        return pl.ds(pl.multiple_of((2 * j + par) * bw + piece * sub, sub), sub)

    def wide(h, r):
        return pl.multiple_of(4 * level(h, r) * bw, 4 * bw)

    xa, xb = [], []
    for u in range(nu):
        mine_at, part_at = cols(t, u, c), cols(t, u, 1 - c)
        src = g_hbm if u < early else za
        xa.append(remote(src.at[:, mine_at], zb.at[:, mine_at], x_s.at[0], x_r.at[u], xpeer))
        if u < early:
            xb.append(remote(src.at[:, part_at], zb.at[:, part_at], x_s.at[1], x_r.at[u], xpeer))
        else:
            xb.append(remote(src.at[:, part_at], zpx.at[u], x_s.at[1], x_r.at[u], (pd, oh)))
    for u in range(early):
        xb[u].start()
        xa[u].start()

    for copy in smalls:
        copy.wait()
    gpad[...] = jnp.zeros_like(gpad)
    gpad[:, :slots] = gate[...].T
    grecv[0] = gpad[...]
    gcopies = [remote(gpad, grecv.at[o], gt_s, gt_r, (peer(o), t)) for o in range(1, n)]
    for copy in gcopies:
        copy.start()
    wcopy = pltpu.make_async_copy(w_hbm, w, w_sem)
    wcopy.start()
    tcopy = remote(attn_hbm, attn_p, t_s, t_r, partner)
    tcopy.start()
    three = split3(rwt[...])
    gcopy.wait()

    def local_step(i, _):
        at = pl.ds(pl.multiple_of(i * tile, tile), tile)
        r = jnp.dot(three, g[:, at], preferred_element_type=F32)
        local[:, at] = r[:slots] + r[slots : 2 * slots] + r[2 * slots :]
        return 0

    lax.fori_loop(0, half // tile, local_step, 0)

    def slab(o):
        return pl.ds(pl.multiple_of(peer(o) * lw, lw), lw)

    lcopies = [
        remote(local.at[:, slab(o)], lrecv.at[o], l_s, l_r, (peer(o), t)) for o in range(1, n)
    ]
    for copy in lcopies:
        copy.start()
    lrecv[0] = local[:, slab(0)]

    place_of = lax.broadcasted_iota(jnp.int32, (seg, slots), 0)
    hit = jnp.where(place_of == wpos[...], 1.0, 0.0)
    onehot[...] = hit.astype(BF16)
    mask[...] = jnp.broadcast_to(jnp.sum(hit, axis=1, keepdims=True), mask.shape)

    def row_step(i, _):
        at = pl.ds(pl.multiple_of(i * tile, tile), tile)
        grow[:, at] = tdot(onehot[...], g[:, at])
        return 0

    lax.fori_loop(0, half // tile, row_step, 0)
    others = pl.ds(1, n - 1)
    all_here(grecv.at[others], gt_r)
    all_here(lrecv.at[others], l_r)

    def acopy(o, target):
        return remote(asend.at[o], arecv.at[o], a_s, a_r, (target, t))

    def sweep(i, carry):
        s = n - 1 - i
        slot = lax.rem(d - s + n, n)
        target = lax.rem(s - d + n, n)
        asend[target] = carry
        gates = grecv[slot]
        fresh = lrecv[slot]
        for k in range(slots):
            fresh = fresh + gates[:, k : k + 1] * carry[k : k + 1, :]

        @pl.when(target != 0)
        def _():
            acopy(target, s).start()

        return fresh

    lax.fori_loop(0, n, sweep, jnp.zeros((slots, lw), F32))
    all_here(arecv.at[others], a_r)
    for o in range(n):
        src = lax.rem(d - o + n, n)
        at = pl.ds(pl.multiple_of(src * lw, lw), lw)
        got = arecv[o] if o else asend[0]
        after[:, at] = got
        rows[:, at] = (grow[:, at] + got).astype(BF16)
    for u in range(early):
        for at in (cols(t, u, 1 - c), cols(t, u, c)):
            copy = remote(rows.at[:, at], rows_x.at[:, at], r_s, r_r, xpeer)
            copy.start()

    def fix(src, new_rows, dst, at):
        picked = jnp.dot(onehot[...], new_rows[:, at], preferred_element_type=F32)
        dst[:, at] = jnp.where(mask[...] > 0.5, picked, src[:, at].astype(F32)).astype(BF16)

    pcopies = [
        remote(za.at[:, cols(t, u, 1 - c)], zp.at[u], p_s, p_r.at[u // (nu - 2)], partner) for u in range(nu)
    ]
    qcopies = []
    groups = [[u] for u in range(early)]
    groups += [list(range(max(early, 2 * ns * r), 2 * ns * (r + 1))) for r in range(zh)]
    groups[-1].pop()
    groups.append([nu - 1])
    group_of = {u: k for k, group in enumerate(groups) for u in group}
    for u in range(nu):
        got = q_r.at[group_of[u]]
        if u < early:
            qcopies.append(remote(zb.at[:, cols(oh, u, 1 - c)], zpx.at[u], q_s, got, partner))
        else:
            qcopies.append(remote(zpx.at[u], zb.at[:, cols(oh, u, c)], q_s, got, partner))

    def blocks(count):
        return zpx.at[pl.ds(0, count)]

    def q_here(u):
        all_here(blocks(len(groups[group_of[u]])), q_r.at[group_of[u]])

    def fix_own(u):
        fix(g, rows, za, cols(t, u, 1 - c))
        fix(g, rows, za, cols(t, u, c))
        pcopies[u].start()
        pair = [] if u < early or u == nu - 2 else [u] if u < nu - 2 else [nu - 2, nu - 1]
        if pair:

            @pl.when(c == 0)
            def _():
                for v in pair:
                    xa[v].start()
                for v in pair:
                    xb[v].start()

            @pl.when(c == 1)
            def _():
                for v in pair:
                    xb[v].start()
                for v in pair:
                    xa[v].start()

    for u in [*range(early, min(early + 2, nu)), *range(early), *range(early + 2, nu)]:
        fix_own(u)


    def slot_of(own, u):
        return (0 if own else nu // 2) + u // 2

    def product(own, u, ht):
        zr, zq, at = (za, zp, cols(t, u, c)) if own else (zb, zpx, cols(oh, u, c))
        return tdot(zr[:, at], attn[:, ht]) + tdot(zq[u], attn_p[:, ht])

    def grad_block(own, u):
        slot = slot_of(own, u)

        def step(m, _):
            ht = pl.ds(pl.multiple_of(m * tile, tile), tile)
            r = product(own, u, ht)
            if is_other(u):
                ysend[slot, :, ht] = r.astype(BF16)
            else:
                kept[slot, :, ht] = r
            return 0

        lax.fori_loop(0, hd // tile, step, 0)
        if is_other(u):
            ycopy(slot, every, slot).start()

    every = pl.ds(0, hd)

    def ycopy(slot, ht, k):
        return remote(ysend.at[slot, :, ht], yrecv.at[slot, :, ht], y_s, y_r.at[k], ypeer)

    def last_sent_block(u):
        slot = slot_of(False, u)
        for k in range(hd // tile):
            ht = pl.ds(k * tile, tile)
            ysend[slot, :, ht] = product(False, u, ht).astype(BF16)
            ycopy(slot, ht, slot + k).start()

    outer = (z == 0) | (z == nz - 1)
    low = z < zh
    inner_z = jnp.where(low, zh - 1, zh)

    def place(own, u):
        zd = zh * (t if own else oh) + level(t if own else oh, u // (2 * ns))
        across = (zd < zh) != low
        return slot_of(own, u), u % (2 * ns) // 2, zd, zd == z, across

    def at_chip(zt):
        return (zt * 4 + 2 * y + c, t)

    def to_relay(slot, ht, k):
        return remote(
            zsend.at[slot, :, ht], zpass.at[slot, :, ht], z_s, v_r.at[slot + k], at_chip(inner_z)
        )

    def to_home(slot, piece, zd, ht, kind):
        return remote(
            zsend.at[slot, :, ht], zrecv.at[kind, piece, :, ht], z_s, z_r.at[kind, piece], at_chip(zd)
        )

    def first_stage(own, u, total, ht, k):
        slot, piece, zd, at_home, across = place(own, u)

        @pl.when(at_home)
        def _():
            mine[piece, :, ht] = total

        @pl.when(across & jnp.logical_not(outer))
        def _():
            kept[slot, :, ht] = total

        @pl.when(across & outer)
        def _():
            zsend[slot, :, ht] = total.astype(BF16)
            to_relay(slot, ht, k).start()

        @pl.when(jnp.logical_not(across | at_home))
        def _():
            zsend[slot, :, ht] = total.astype(BF16)
            to_home(slot, piece, zd, ht, 1).start()

    def second_stage(own, u, ht, k):
        slot, piece, zd, _, across = place(own, u)

        @pl.when(across & jnp.logical_not(outer))
        def _():
            to_relay(slot, ht, k).wait_recv()
            zsend[slot, :, ht] = (kept[slot, :, ht] + zpass[slot, :, ht].astype(F32)).astype(BF16)
            to_home(slot, piece, zd, ht, 0).start()

    def to_owner(own, u):
        slot = slot_of(own, u)
        ycopy(slot, every, slot).wait_recv()
        first_stage(own, u, kept[slot] + yrecv[slot].astype(F32), every, 0)

    def last_block(u):
        slot = slot_of(False, u)
        for k in range(hd // tile):
            ht = pl.ds(k * tile, tile)
            total = product(False, u, ht)
            ycopy(slot, ht, slot + k).wait_recv()
            first_stage(False, u, total + yrecv[slot, :, ht].astype(F32), ht, k)

    def pass_on(own, u):
        if not own and u == nu - 1:
            for k in range(hd // tile):
                second_stage(own, u, pl.ds(k * tile, tile), k)
        else:
            second_stage(own, u, every, 0)

    def own_attn():
        wcopy.wait()

        def step(m, _):
            at = pl.ds(pl.multiple_of(m * tile, tile), tile)
            k = pl.ds(pl.multiple_of(t * half, half), half)
            acc[:, at] = jnp.dot(za[...], w[k, at], preferred_element_type=F32)
            return 0

        lax.fori_loop(0, hd // tile, step, 0)

    def other_attn(r):
        from_at = wide(oh, r)
        if 2 * ns * (r + 1) > early:
            q_here(2 * ns * (r + 1) - 1)

        def step(m, _):
            at = pl.ds(pl.multiple_of(m * tile, tile), tile)
            k = pl.ds(pl.multiple_of(oh * half + from_at, 4 * bw), 4 * bw)
            total = acc[:, at] + jnp.dot(
                zb[:, pl.ds(from_at, 4 * bw)], w[k, at], preferred_element_type=F32
            )
            acc[:, at] = total
            return 0

        lax.fori_loop(0, hd // tile, step, 0)

    def part_attn(units):
        q_here(units[-1])
        places = [cols(oh, u, par) for u in units for par in range(2)]

        def step(m, _):
            at = pl.ds(pl.multiple_of(m * tile, tile), tile)
            lhs = jnp.concatenate([zb[:, k] for k in places], axis=1)
            rhs = jnp.concatenate(
                [w[pl.ds(pl.multiple_of(oh * half + k.start, sub), sub), at] for k in places], axis=0
            )
            total = acc[:, at] + jnp.dot(lhs, rhs, preferred_element_type=F32)
            if nu - 1 in units:
                out_attn[:, at] = total.astype(BF16)
            else:
                acc[:, at] = total
            return 0

        lax.fori_loop(0, hd // tile, step, 0)

    def memory():
        gates = gpad[...]

        def step(i, _):
            at = pl.ds(pl.multiple_of(i * tile, tile), tile)
            fresh = local[:, at]
            carry = after[:, at]
            for k in range(slots):
                fresh = fresh + gates[:, k : k + 1] * carry[k : k + 1, :]
            out_mem[:, at] = fresh
            return 0

        lax.fori_loop(0, half // tile, step, 0)

    attncopy.wait()
    tcopy.wait_recv()
    for kind, u in plan(nu, ns, early):
        if kind == "own":
            if u == 0:
                all_here(blocks(nu - 2), p_r.at[0])
            if u == nu - 2:
                all_here(blocks(2), p_r.at[1])
            grad_block(True, u)
        elif kind == "prep":
            if u == 0:
                all_here(rows_x.at[:, pl.ds(0, 2 * early * sub)], r_r)
            all_here(blocks(2), x_r.at[u])
            fix(zb, rows_x, zb, cols(oh, u, 1 - c))
            qcopies[u].start()
            fix(zb, rows_x, zb, cols(oh, u, c))
        elif kind == "other":
            if u < early:
                q_here(u)
            else:
                all_here(blocks(2), x_r.at[u])
                qcopies[u].start()
            if u < nu - 2:
                grad_block(False, u)
            elif u < nu - 1:
                last_sent_block(u)
            else:
                last_block(u)
        elif kind == "own_out":
            to_owner(True, u)
        elif kind in ("own_pass", "other_pass"):
            pass_on(kind == "own_pass", u)
        elif kind == "other_out":
            to_owner(False, u)
        elif kind == "own_attn":
            own_attn()
        elif kind == "attn":
            other_attn(u)
        elif kind == "attn_part":
            part_attn(u)
        elif kind in ("attn_part0", "attn_part1"):

            @pl.when(c == int(kind[-1]))
            def _(u=u):
                part_attn(u)

        else:
            memory()

    for piece in range(ns):
        total = mine[piece]
        for kind in range(2):
            to_home(0, piece, z, every, kind).wait_recv()
            total = total + zrecv[kind, piece].astype(F32)
        out_w[pl.ds(piece * sub, sub), :] = total

    all_sent(zp, x_s.at[0])
    all_sent(zp, x_s.at[1])
    all_sent(zp, p_s)
    all_sent(zp, q_s)
    all_sent(grecv.at[others], gt_s)
    all_sent(lrecv.at[others], l_s)
    all_sent(arecv.at[others], a_s)
    all_sent(rows.at[:, pl.ds(0, 2 * early * sub)], r_s)
    all_sent(yrecv, y_s)
    all_sent(zsend.at[pl.ds(0, nu - ns)], z_s)
    tcopy.wait_send()


def settle_kernel(a, b, m, out_a, out_b, out_m, sems):
    copies = [
        pltpu.make_async_copy(src, dst, sems.at[i])
        for i, (src, dst) in enumerate(((a, out_a), (b, out_b), (m, out_m)))
    ]
    for copy in copies:
        copy.start()
    for copy in copies:
        copy.wait()


def settled(outs):
    return pl.pallas_call(
        settle_kernel,
        out_shape=tuple(jax.ShapeDtypeStruct(o.shape, o.dtype) for o in outs),
        in_specs=[pl.BlockSpec(memory_space=pltpu.VMEM)] * 3,
        out_specs=tuple([pl.BlockSpec(memory_space=pl.ANY)] * 3),
        scratch_shapes=[pltpu.SemaphoreType.DMA((3,))],
    )(*[pltpu.with_memory_space_constraint(o, pltpu.VMEM) for o in outs])


def fused(n, attn_out, out_proj_t, grad_out, read_weights, memory_gate, write_pos):
    seg, half = grad_out.shape
    hd = attn_out.shape[1]
    slots = write_pos.shape[1]
    depth = out_proj_t.shape[0]
    bw, lw, nz = depth // n, half // n, n // 4
    sub = 128
    ns = bw // sub
    nu = nz * ns
    zh = nz // 2
    early = EARLY
    V = pltpu.VMEM
    D = pltpu.SemaphoreType.DMA
    vmem = pl.BlockSpec(memory_space=pltpu.VMEM)
    outs = pl.pallas_call(
        functools.partial(kernel, n, early),
        out_shape=(V((seg, hd), BF16), V((bw, hd), F32), V((slots, half), F32)),
        in_specs=[pl.BlockSpec(memory_space=pl.ANY)] * 6,
        out_specs=(vmem, vmem, vmem),
        scratch_shapes=[
            V((slots, seg), F32),
            V((slots, slots), F32),
            V((1, slots), jnp.int32),
            V((seg, half), BF16),
            V((seg, hd), BF16),
            V((depth, hd), BF16),
            V((seg, hd), BF16),
            V((seg, half), BF16),
            V((seg, half), BF16),
            V((nu, seg, sub), BF16),
            V((nu, seg, sub), BF16),
            V((seg, hd), F32),
            V((seg, slots), BF16),
            V((seg, sub), F32),
            V((slots, half), F32),
            V((slots, half), BF16),
            V((slots, half), BF16),
            V((slots, half), F32),
            V((slots, half), F32),
            V((slots, 128), F32),
            V((n, slots, 128), F32),
            V((n, slots, lw), F32),
            V((n, slots, lw), F32),
            V((n, slots, lw), F32),
            V((nu, sub, hd), BF16),
            V((nu, sub, hd), BF16),
            V((nu, sub, hd), F32),
            V((nu, sub, hd), BF16),
            V((nu, sub, hd), BF16),
            V((2, ns, sub, hd), BF16),
            V((ns, sub, hd), F32),
            D((3,)),
            D,
            D,
            D,
            D((2,)),
            D((nu,)),
            D,
            D,
            D,
            D,
            D,
            D,
            D,
            D,
            D,
            D,
            D,
            D((2,)),
            D,
            D((early + zh + 1,)),
            D,
            D((nu - 1 + hd // 256,)),
            D,
            D((nu - 1 + hd // 256,)),
            D((2, ns)),
        ],
        compiler_params=pltpu.CompilerParams(
            collective_id=0, has_side_effects=True, vmem_limit_bytes=52 * 1024 * 1024
        ),
    )(attn_out, out_proj_t, grad_out, read_weights.T, memory_gate, write_pos)
    return settled(outs)


def plain(attn_out, out_proj_t, grad_out, read_weights, memory_gate, write_pos):
    high = lax.Precision.HIGHEST
    seg_len = attn_out.shape[0]
    slots = write_pos.shape[1]
    gate_at_step = memory_gate.T
    dy_cols = grad_out.astype(jnp.float32)
    local = jnp.dot(read_weights.T, dy_cols, precision=high, preferred_element_type=jnp.float32)
    all_gates, all_terms = (
        lax.all_gather(gate_at_step, "dp", axis=0, tiled=True),
        lax.all_gather(local, "dp", axis=0, tiled=True),
    )
    count = lax.axis_size("dp")
    mine = lax.axis_index("dp")

    def sweep(step, carry):
        which = (count - 1 - step).astype(jnp.int32)
        gate = lax.dynamic_slice_in_dim(all_gates, which * slots, slots, 0)
        term = lax.dynamic_slice_in_dim(all_terms, which * slots, slots, 0)
        fresh = jnp.dot(gate, carry, precision=high, preferred_element_type=jnp.float32) + term
        return jnp.where(which > mine, fresh, carry)

    after = lax.fori_loop(0, count, sweep, jnp.zeros_like(local))
    grad_memory = (
        jnp.dot(gate_at_step, after, precision=high, preferred_element_type=jnp.float32) + local
    )
    places = jnp.arange(seg_len, dtype=jnp.int32)
    onehot = (places[:, None] == write_pos[0][None, :]).astype(jnp.float32)
    written = jnp.dot(onehot, after, precision=high, preferred_element_type=jnp.float32)
    grad_z = (dy_cols + written).astype(jnp.bfloat16)
    full_z = lax.all_gather(grad_z, "tensor", axis=1, tiled=True)
    grad_attn = jnp.dot(full_z, out_proj_t, preferred_element_type=jnp.float32).astype(jnp.bfloat16)
    term = lax.dot_general(
        full_z, attn_out, (((0,), (0,)), ((), ())), preferred_element_type=jnp.float32
    )
    grad_weight = lax.psum_scatter(term, "dp", scatter_dimension=0, tiled=True)
    return (grad_attn, grad_weight, grad_memory)


def solution(mesh):
    n = mesh.shape["dp"]
    parts = mesh.shape["tensor"]

    def body(attn_out, out_proj_t, grad_out, read_weights, memory_gate, write_pos):
        half, hd = grad_out.shape[1], attn_out.shape[1]
        fits = (
            parts == 2
            and n // 4 == 4
            and half % (n * 128) == 0
            and half % 256 == 0
            and hd % 256 == 0
            and out_proj_t.shape[0] <= 4096
        )
        args = (attn_out, out_proj_t, grad_out, read_weights, memory_gate, write_pos)
        return fused(n, *args) if fits else plain(*args)

    return jax.shard_map(
        body,
        mesh=mesh,
        in_specs=(
            P("dp", "tensor"),
            P(None, "tensor"),
            P("dp", "tensor"),
            P("dp", None),
            P("dp", None),
            P("dp", None),
        ),
        out_specs=(P("dp", "tensor"), P("dp", "tensor"), P("dp", "tensor")),
        check_vma=False,
    )
```

```python
import functools

import jax
import jax.numpy as jnp
from jax import lax
from jax.experimental import pallas as pl
from jax.experimental.pallas import tpu as pltpu
from jax.sharding import PartitionSpec as P

MESH = pl.DeviceIdType.MESH
F32 = jnp.float32
BF16 = jnp.bfloat16
EARLY = 2
PARTS = 1


def split3(a):
    hi = a.astype(BF16)
    rest = a - hi.astype(F32)
    mid = rest.astype(BF16)
    low = (rest - mid.astype(F32)).astype(BF16)
    return jnp.concatenate([hi, mid, low], axis=0)


def tdot(a, b):
    return lax.dot_general(a, b, (((0,), (0,)), ((), ())), preferred_element_type=F32)


def plan(nu, ns, early):
    steps = []
    for u in range(nu):
        lead = u < nu // 2
        own = 2.0 + 0.2 * u if lead else (3.05 + 0.05 * (u - nu // 2) if u < nu - 2 else 5.15 + 0.05 * (u + 2 - nu))
        steps.append((own, "own", u))
        if u < early:
            steps.append((early + 0.1 + 0.25 * u, "prep", u))
            arrived = early + 0.2 + 0.25 * u
        else:
            arrived = u + 1.0
        steps.append((arrived, "other", u))
        if u % 2:
            sent = max(own + 0.01, 3.05 + 0.67 * (u - 1))
            steps.append((sent, "own_out", u))
            steps.append((sent + 1.3, "own_pass", u))
            sent = max(arrived + 0.01, 3.7 + 0.66 * (u - 1))
            if u < nu - 1:
                steps.append((sent, "other_out", u))
            steps.append((sent + (1.2 if u < nu - 1 else 0.1), "other_pass", u))
        if (u + 1) % (2 * ns) == 0 and u < nu - 1:
            steps.append((arrived + 1.5, "attn", u // (2 * ns)))
        if u == nu - 2:
            steps.append((arrived - 0.6, "attn_part", range(nu - 2 * ns, u)))
            steps.append((arrived + 0.2, "attn_part1", [u]))
        if u == nu - 1:
            steps.append((arrived + 1.0, "attn_part0", [u - 1]))
            steps.append((arrived + 1.1, "attn_part", [u]))
    steps.append((4.2, "own_attn", 0))
    steps.append((4.25, "memory", 0))
    return [step[1:] for step in sorted(steps, key=lambda step: step[0])]


def kernel(
    n, early, attn_hbm, w_hbm, g_hbm, rwt_hbm, gate_hbm, wpos_hbm, out_attn, out_w, out_mem,
    rwt, gate, wpos, g, attn, w, attn_p, za, zb, zp, zpx, acc, onehot, mask, grow, rows, early_rows, rows_x, local, after,
    gpad, grecv, lrecv, asend, arecv, ysend, yrecv, kept, zsend, zpass, zrecv, mine,
    small_sem, g_sem, attn_sem, w_sem, x_s, x_r, gt_s, gt_r, l_s, l_r, a_s, a_r, r_s, r_r, t_s, t_r,
    p_s, p_r, q_s, q_r, y_s, y_r, z_s, v_r, z_r,
):
    d = lax.axis_index("dp")
    t = lax.axis_index("tensor")
    c = lax.rem(d, 2)
    y = lax.rem(d // 2, 2)
    z = d // 4
    nz = n // 4
    seg, half = g.shape
    hd = attn.shape[1]
    slots = rwt.shape[0]
    bw = 2 * half // n
    lw = half // n
    zh = nz // 2
    sub = mask.shape[1]
    ns = bw // sub
    nu = 2 * zh * ns
    oh = 1 - t
    pd = d + 1 - 2 * c
    partner = (pd, t)
    xpeer = (d, oh)
    ypeer = (d + 2 - 4 * y, t)
    tile = 256

    def remote(src, dst, ss, rs, dev):
        return pltpu.make_async_remote_copy(
            src_ref=src, dst_ref=dst, send_sem=ss, recv_sem=rs, device_id=dev, device_id_type=MESH
        )

    def all_sent(ref, sem):
        remote(ref, ref, sem, sem, xpeer).wait_send()

    def all_here(ref, sem):
        remote(ref, ref, sem, sem, xpeer).wait_recv()

    def peer(o):
        return lax.rem(d + o, n)

    barrier = pltpu.get_barrier_semaphore()
    for o in range(1, n):
        pl.semaphore_signal(barrier, inc=1, device_id=(peer(o), t), device_id_type=MESH)
    pl.semaphore_signal(barrier, inc=1, device_id=xpeer, device_id_type=MESH)
    pl.semaphore_signal(barrier, inc=1, device_id=(pd, oh), device_id_type=MESH)

    smalls = [
        pltpu.make_async_copy(src, dst, small_sem.at[i])
        for i, (src, dst) in enumerate(((rwt_hbm, rwt), (gate_hbm, gate), (wpos_hbm, wpos)))
    ]
    for copy in smalls:
        copy.start()
    gcopy = pltpu.make_async_copy(g_hbm, g, g_sem)
    gcopy.start()
    attncopy = pltpu.make_async_copy(attn_hbm, attn, attn_sem)
    pl.semaphore_wait(barrier, n + 1)

    def is_other(u):
        return u % 2 == 0

    def level(h, r):
        return r + h * (zh - 1 - 2 * r)

    def cols(h, u, par):
        yd = 1 - y if is_other(u) else y
        j = 2 * level(h, u // (2 * ns)) + yd
        piece = u % (2 * ns) // 2
        return pl.ds(pl.multiple_of((2 * j + par) * bw + piece * sub, sub), sub)

    def wide(h, r):
        return pl.multiple_of(4 * level(h, r) * bw, 4 * bw)

    xa, xb = [], []
    for u in range(nu):
        mine_at, part_at = cols(t, u, c), cols(t, u, 1 - c)
        src = g if u < early else za
        xa.append(remote(src.at[:, mine_at], zb.at[:, mine_at], x_s.at[0], x_r.at[u], xpeer))
        if u < early:
            xb.append(remote(src.at[:, part_at], zb.at[:, part_at], x_s.at[1], x_r.at[u], xpeer))
        else:
            xb.append(remote(src.at[:, part_at], zpx.at[u], x_s.at[1], x_r.at[u], (pd, oh)))
    gcopy.wait()
    for u in range(early):
        xb[u].start()
        xa[u].start()

    for copy in smalls:
        copy.wait()
    gpad[...] = jnp.zeros_like(gpad)
    gpad[:, :slots] = gate[...].T
    grecv[0] = gpad[...]
    gcopies = [remote(gpad, grecv.at[o], gt_s, gt_r, (peer(o), t)) for o in range(1, n)]
    for copy in gcopies:
        copy.start()
    wcopy = pltpu.make_async_copy(w_hbm, w, w_sem)
    tcopy = remote(attn_hbm, attn_p, t_s, t_r, partner)
    three = split3(rwt[...])

    def local_step(i, _):
        at = pl.ds(pl.multiple_of(i * tile, tile), tile)
        r = jnp.dot(three, g[:, at], preferred_element_type=F32)
        local[:, at] = r[:slots] + r[slots : 2 * slots] + r[2 * slots :]
        return 0

    lax.fori_loop(0, half // tile, local_step, 0)

    def slab(o):
        return pl.ds(pl.multiple_of(peer(o) * lw, lw), lw)

    lcopies = [
        remote(local.at[:, slab(o)], lrecv.at[o], l_s, l_r, (peer(o), t)) for o in range(1, n)
    ]
    for copy in lcopies:
        copy.start()
    lrecv[0] = local[:, slab(0)]
    attncopy.start()
    tcopy.start()

    place_of = lax.broadcasted_iota(jnp.int32, (seg, slots), 0)
    hit = jnp.where(place_of == wpos[...], 1.0, 0.0)
    onehot[...] = hit.astype(BF16)
    mask[...] = jnp.broadcast_to(jnp.sum(hit, axis=1, keepdims=True), mask.shape)

    def row_step(i, _):
        at = pl.ds(pl.multiple_of(i * tile, tile), tile)
        grow[:, at] = tdot(onehot[...], g[:, at])
        return 0

    lax.fori_loop(0, half // tile, row_step, 0)
    others = pl.ds(1, n - 1)
    all_here(grecv.at[others], gt_r)
    all_here(lrecv.at[others], l_r)

    def acopy(o, target):
        return remote(asend.at[o], arecv.at[o], a_s, a_r, (target, t))

    def sweep(i, carry):
        s = n - 1 - i
        slot = lax.rem(d - s + n, n)
        target = lax.rem(s - d + n, n)
        asend[target] = carry
        gates = grecv[slot]
        fresh = lrecv[slot]
        for k in range(slots):
            fresh = fresh + gates[:, k : k + 1] * carry[k : k + 1, :]

        @pl.when(target != 0)
        def _():
            acopy(target, s).start()

        return fresh

    lax.fori_loop(0, n, sweep, jnp.zeros((slots, lw), F32))
    wcopy.start()
    all_here(arecv.at[others], a_r)
    for o in range(n):
        src = lax.rem(d - o + n, n)
        at = pl.ds(pl.multiple_of(src * lw, lw), lw)
        got = arecv[o] if o else asend[0]
        after[:, at] = got
        rows[:, at] = (grow[:, at] + got).astype(BF16)
    for u in range(early):
        for k, at in enumerate((cols(t, u, 1 - c), cols(t, u, c))):
            early_rows[:, pl.ds((2 * u + k) * sub, sub)] = rows[:, at]
    rcopy = remote(early_rows, rows_x, r_s, r_r, xpeer)
    rcopy.start()

    def fix(src, new_rows, dst, at):
        picked = jnp.dot(onehot[...], new_rows, preferred_element_type=F32)
        dst[:, at] = jnp.where(mask[...] > 0.5, picked, src[:, at].astype(F32)).astype(BF16)

    pcopies = [
        remote(za.at[:, cols(t, u, 1 - c)], zp.at[u], p_s, p_r.at[u // (nu - 2)], partner) for u in range(nu)
    ]
    qcopies = []
    groups = [[u] for u in range(early)]
    groups += [list(range(max(early, 2 * ns * r), 2 * ns * (r + 1))) for r in range(zh)]
    groups[-1] = groups[-1][:-2]
    groups += [[nu - 2], [nu - 1]]
    group_of = {u: k for k, group in enumerate(groups) for u in group}
    for u in range(nu):
        got = q_r.at[group_of[u]]
        if u < early:
            qcopies.append(remote(zb.at[:, cols(oh, u, 1 - c)], zpx.at[u], q_s, got, partner))
        else:
            qcopies.append(remote(zpx.at[u], zb.at[:, cols(oh, u, c)], q_s, got, partner))

    def blocks(count):
        return zpx.at[pl.ds(0, count)]

    def q_here(u):
        all_here(blocks(len(groups[group_of[u]])), q_r.at[group_of[u]])

    def fix_own(u):
        for at in (cols(t, u, 1 - c), cols(t, u, c)):
            fix(g, rows[:, at], za, at)
        pcopies[u].start()
        pair = [] if u < early or u == nu - 2 else [u] if u < nu - 2 else [nu - 2, nu - 1]
        if pair:

            @pl.when(c == 0)
            def _():
                for v in pair:
                    xa[v].start()
                for v in pair:
                    xb[v].start()

            @pl.when(c == 1)
            def _():
                for v in pair:
                    xb[v].start()
                for v in pair:
                    xa[v].start()

    for u in [*range(early, min(early + 2, nu)), *range(early), *range(early + 2, nu)]:
        fix_own(u)


    def slot_of(own, u):
        return (0 if own else nu // 2) + u // 2

    def product(own, u, ht):
        zr, zq, at = (za, zp, cols(t, u, c)) if own else (zb, zpx, cols(oh, u, c))
        return tdot(zr[:, at], attn[:, ht]) + tdot(zq[u], attn_p[:, ht])

    def grad_block(own, u):
        slot = slot_of(own, u)

        def step(m, _):
            ht = pl.ds(pl.multiple_of(m * tile, tile), tile)
            r = product(own, u, ht)
            if is_other(u):
                ysend[slot, :, ht] = r.astype(BF16)
            else:
                kept[slot, :, ht] = r
            return 0

        lax.fori_loop(0, hd // tile, step, 0)
        if is_other(u):
            ycopy(slot, every, slot).start()

    every = pl.ds(0, hd)

    def ycopy(slot, ht, k):
        return remote(ysend.at[slot, :, ht], yrecv.at[slot, :, ht], y_s, y_r.at[k], ypeer)

    def last_sent_block(u):
        slot = slot_of(False, u)
        for k in range(hd // tile):
            ht = pl.ds(k * tile, tile)
            ysend[slot, :, ht] = product(False, u, ht).astype(BF16)
            ycopy(slot, ht, slot + k).start()

    outer = (z == 0) | (z == nz - 1)
    low = z < zh
    inner_z = jnp.where(low, zh - 1, zh)

    def place(own, u):
        zd = zh * (t if own else oh) + level(t if own else oh, u // (2 * ns))
        across = (zd < zh) != low
        return slot_of(own, u), u % (2 * ns) // 2, zd, zd == z, across

    def at_chip(zt):
        return (zt * 4 + 2 * y + c, t)

    def to_relay(slot, ht, k):
        return remote(
            zsend.at[slot, :, ht], zpass.at[slot, :, ht], z_s, v_r.at[slot + k], at_chip(inner_z)
        )

    def to_home(slot, piece, zd, ht, kind):
        return remote(
            zsend.at[slot, :, ht], zrecv.at[kind, piece, :, ht], z_s, z_r.at[kind, piece], at_chip(zd)
        )

    def first_stage(own, u, total, ht, k):
        slot, piece, zd, at_home, across = place(own, u)

        @pl.when(at_home)
        def _():
            mine[piece, :, ht] = total

        @pl.when(across & jnp.logical_not(outer))
        def _():
            kept[slot, :, ht] = total

        @pl.when(across & outer)
        def _():
            zsend[slot, :, ht] = total.astype(BF16)
            to_relay(slot, ht, k).start()

        @pl.when(jnp.logical_not(across | at_home))
        def _():
            zsend[slot, :, ht] = total.astype(BF16)
            to_home(slot, piece, zd, ht, 1).start()

    def second_stage(own, u, ht, k):
        slot, piece, zd, _, across = place(own, u)

        @pl.when(across & jnp.logical_not(outer))
        def _():
            to_relay(slot, ht, k).wait_recv()
            zsend[slot, :, ht] = (kept[slot, :, ht] + zpass[slot, :, ht].astype(F32)).astype(BF16)
            to_home(slot, piece, zd, ht, 0).start()

    def to_owner(own, u):
        slot = slot_of(own, u)
        ycopy(slot, every, slot).wait_recv()
        first_stage(own, u, kept[slot] + yrecv[slot].astype(F32), every, 0)

    def last_block(u):
        slot = slot_of(False, u)
        for k in range(hd // tile):
            ht = pl.ds(k * tile, tile)
            total = product(False, u, ht)
            ycopy(slot, ht, slot + k).wait_recv()
            first_stage(False, u, total + yrecv[slot, :, ht].astype(F32), ht, k)

    def pass_on(own, u):
        if not own and u == nu - 1:
            for k in range(hd // tile):
                second_stage(own, u, pl.ds(k * tile, tile), k)
        else:
            second_stage(own, u, every, 0)

    def own_attn():
        wcopy.wait()

        def step(m, _):
            at = pl.ds(pl.multiple_of(m * tile, tile), tile)
            k = pl.ds(pl.multiple_of(t * half, half), half)
            acc[:, at] = jnp.dot(za[...], w[k, at], preferred_element_type=F32)
            return 0

        lax.fori_loop(0, hd // tile, step, 0)

    def other_attn(r):
        from_at = wide(oh, r)
        if 2 * ns * (r + 1) > early:
            q_here(2 * ns * (r + 1) - 1)

        def step(m, _):
            at = pl.ds(pl.multiple_of(m * tile, tile), tile)
            k = pl.ds(pl.multiple_of(oh * half + from_at, 4 * bw), 4 * bw)
            total = acc[:, at] + jnp.dot(
                zb[:, pl.ds(from_at, 4 * bw)], w[k, at], preferred_element_type=F32
            )
            acc[:, at] = total
            return 0

        lax.fori_loop(0, hd // tile, step, 0)

    def part_attn(units):
        q_here(units[-1])
        places = [cols(oh, u, par) for u in units for par in range(2)]

        def step(m, _):
            at = pl.ds(pl.multiple_of(m * tile, tile), tile)
            lhs = jnp.concatenate([zb[:, k] for k in places], axis=1)
            rhs = jnp.concatenate(
                [w[pl.ds(pl.multiple_of(oh * half + k.start, sub), sub), at] for k in places], axis=0
            )
            total = acc[:, at] + jnp.dot(lhs, rhs, preferred_element_type=F32)
            if nu - 1 in units:
                out_attn[:, at] = total.astype(BF16)
            else:
                acc[:, at] = total
            return 0

        lax.fori_loop(0, hd // tile, step, 0)

    def memory():
        gates = gpad[...]

        def step(i, _):
            at = pl.ds(pl.multiple_of(i * tile, tile), tile)
            fresh = local[:, at]
            carry = after[:, at]
            for k in range(slots):
                fresh = fresh + gates[:, k : k + 1] * carry[k : k + 1, :]
            out_mem[:, at] = fresh
            return 0

        lax.fori_loop(0, half // tile, step, 0)

    attncopy.wait()
    tcopy.wait_recv()
    for kind, u in plan(nu, ns, early):
        if kind == "own":
            if u == 0:
                all_here(blocks(nu - 2), p_r.at[0])
            if u == nu - 2:
                all_here(blocks(2), p_r.at[1])
            grad_block(True, u)
        elif kind == "prep":
            if u == 0:
                rcopy.wait_recv()
            all_here(blocks(2), x_r.at[u])
            fix(zb, rows_x[:, pl.ds(2 * u * sub, sub)], zb, cols(oh, u, 1 - c))
            qcopies[u].start()
            fix(zb, rows_x[:, pl.ds((2 * u + 1) * sub, sub)], zb, cols(oh, u, c))
        elif kind == "other":
            if u < early:
                q_here(u)
            else:
                all_here(blocks(2), x_r.at[u])
                qcopies[u].start()
            if u < nu - 2:
                grad_block(False, u)
            elif u < nu - 1:
                last_sent_block(u)
            else:
                last_block(u)
        elif kind == "own_out":
            to_owner(True, u)
        elif kind in ("own_pass", "other_pass"):
            pass_on(kind == "own_pass", u)
        elif kind == "other_out":
            to_owner(False, u)
        elif kind == "own_attn":
            own_attn()
        elif kind == "attn":
            other_attn(u)
        elif kind == "attn_part":
            part_attn(u)
        elif kind in ("attn_part0", "attn_part1"):

            @pl.when(c == int(kind[-1]))
            def _(u=u):
                part_attn(u)

        else:
            memory()

    for piece in range(ns):
        total = mine[piece]
        for kind in range(2):
            to_home(0, piece, z, every, kind).wait_recv()
            total = total + zrecv[kind, piece].astype(F32)
        out_w[pl.ds(piece * sub, sub), :] = total

    all_sent(zp, x_s.at[0])
    all_sent(zp, x_s.at[1])
    all_sent(zp, p_s)
    all_sent(zp, q_s)
    all_sent(grecv.at[others], gt_s)
    all_sent(lrecv.at[others], l_s)
    all_sent(arecv.at[others], a_s)
    rcopy.wait_send()
    all_sent(yrecv, y_s)
    all_sent(zsend.at[pl.ds(0, nu - ns)], z_s)
    tcopy.wait_send()


def settle_kernel(a, b, m, out_a, out_b, out_m, sems):
    copies = []
    for src, dst, parts in ((a, out_a, PARTS), (b, out_b, PARTS), (m, out_m, 1)):
        rows = src.shape[0] // parts
        for i in range(parts):
            at = pl.ds(i * rows, rows)
            copies.append(pltpu.make_async_copy(src.at[at], dst.at[at], sems.at[len(copies)]))
    for copy in copies:
        copy.start()
    for copy in copies:
        copy.wait()


def settled(outs):
    return pl.pallas_call(
        settle_kernel,
        out_shape=tuple(jax.ShapeDtypeStruct(o.shape, o.dtype) for o in outs),
        in_specs=[pl.BlockSpec(memory_space=pltpu.VMEM)] * 3,
        out_specs=tuple([pl.BlockSpec(memory_space=pl.ANY)] * 3),
        scratch_shapes=[pltpu.SemaphoreType.DMA((2 * PARTS + 1,))],
    )(*[pltpu.with_memory_space_constraint(o, pltpu.VMEM) for o in outs])


def fused(n, attn_out, out_proj_t, grad_out, read_weights, memory_gate, write_pos):
    seg, half = grad_out.shape
    hd = attn_out.shape[1]
    slots = write_pos.shape[1]
    depth = out_proj_t.shape[0]
    bw, lw, nz = depth // n, half // n, n // 4
    sub = 128
    ns = bw // sub
    nu = nz * ns
    zh = nz // 2
    early = EARLY
    V = pltpu.VMEM
    D = pltpu.SemaphoreType.DMA
    vmem = pl.BlockSpec(memory_space=pltpu.VMEM)
    outs = pl.pallas_call(
        functools.partial(kernel, n, early),
        out_shape=(V((seg, hd), BF16), V((bw, hd), F32), V((slots, half), F32)),
        in_specs=[pl.BlockSpec(memory_space=pl.ANY)] * 6,
        out_specs=(vmem, vmem, vmem),
        scratch_shapes=[
            V((slots, seg), F32),
            V((slots, slots), F32),
            V((1, slots), jnp.int32),
            V((seg, half), BF16),
            V((seg, hd), BF16),
            V((depth, hd), BF16),
            V((seg, hd), BF16),
            V((seg, half), BF16),
            V((seg, half), BF16),
            V((nu, seg, sub), BF16),
            V((nu, seg, sub), BF16),
            V((seg, hd), F32),
            V((seg, slots), BF16),
            V((seg, sub), F32),
            V((slots, half), F32),
            V((slots, half), BF16),
            V((slots, 2 * early * sub), BF16),
            V((slots, 2 * early * sub), BF16),
            V((slots, half), F32),
            V((slots, half), F32),
            V((slots, 128), F32),
            V((n, slots, 128), F32),
            V((n, slots, lw), F32),
            V((n, slots, lw), F32),
            V((n, slots, lw), F32),
            V((nu, sub, hd), BF16),
            V((nu, sub, hd), BF16),
            V((nu, sub, hd), F32),
            V((nu, sub, hd), BF16),
            V((nu, sub, hd), BF16),
            V((2, ns, sub, hd), BF16),
            V((ns, sub, hd), F32),
            D((3,)),
            D,
            D,
            D,
            D((2,)),
            D((nu,)),
            D,
            D,
            D,
            D,
            D,
            D,
            D,
            D,
            D,
            D,
            D,
            D((2,)),
            D,
            D((early + zh + 2,)),
            D,
            D((nu - 1 + hd // 256,)),
            D,
            D((nu - 1 + hd // 256,)),
            D((2, ns)),
        ],
        compiler_params=pltpu.CompilerParams(
            collective_id=0, has_side_effects=True, vmem_limit_bytes=52 * 1024 * 1024
        ),
    )(attn_out, out_proj_t, grad_out, read_weights.T, memory_gate, write_pos)
    return settled(outs)


def plain(attn_out, out_proj_t, grad_out, read_weights, memory_gate, write_pos):
    high = lax.Precision.HIGHEST
    seg_len = attn_out.shape[0]
    slots = write_pos.shape[1]
    gate_at_step = memory_gate.T
    dy_cols = grad_out.astype(jnp.float32)
    local = jnp.dot(read_weights.T, dy_cols, precision=high, preferred_element_type=jnp.float32)
    all_gates, all_terms = (
        lax.all_gather(gate_at_step, "dp", axis=0, tiled=True),
        lax.all_gather(local, "dp", axis=0, tiled=True),
    )
    count = lax.axis_size("dp")
    mine = lax.axis_index("dp")

    def sweep(step, carry):
        which = (count - 1 - step).astype(jnp.int32)
        gate = lax.dynamic_slice_in_dim(all_gates, which * slots, slots, 0)
        term = lax.dynamic_slice_in_dim(all_terms, which * slots, slots, 0)
        fresh = jnp.dot(gate, carry, precision=high, preferred_element_type=jnp.float32) + term
        return jnp.where(which > mine, fresh, carry)

    after = lax.fori_loop(0, count, sweep, jnp.zeros_like(local))
    grad_memory = (
        jnp.dot(gate_at_step, after, precision=high, preferred_element_type=jnp.float32) + local
    )
    places = jnp.arange(seg_len, dtype=jnp.int32)
    onehot = (places[:, None] == write_pos[0][None, :]).astype(jnp.float32)
    written = jnp.dot(onehot, after, precision=high, preferred_element_type=jnp.float32)
    grad_z = (dy_cols + written).astype(jnp.bfloat16)
    full_z = lax.all_gather(grad_z, "tensor", axis=1, tiled=True)
    grad_attn = jnp.dot(full_z, out_proj_t, preferred_element_type=jnp.float32).astype(jnp.bfloat16)
    term = lax.dot_general(
        full_z, attn_out, (((0,), (0,)), ((), ())), preferred_element_type=jnp.float32
    )
    grad_weight = lax.psum_scatter(term, "dp", scatter_dimension=0, tiled=True)
    return (grad_attn, grad_weight, grad_memory)


def solution(mesh):
    n = mesh.shape["dp"]
    parts = mesh.shape["tensor"]

    def body(attn_out, out_proj_t, grad_out, read_weights, memory_gate, write_pos):
        half, hd = grad_out.shape[1], attn_out.shape[1]
        fits = (
            parts == 2
            and n // 4 == 4
            and half % (n * 128) == 0
            and half % 256 == 0
            and hd % 256 == 0
            and out_proj_t.shape[0] <= 4096
        )
        args = (attn_out, out_proj_t, grad_out, read_weights, memory_gate, write_pos)
        return fused(n, *args) if fits else plain(*args)

    return jax.shard_map(
        body,
        mesh=mesh,
        in_specs=(
            P("dp", "tensor"),
            P(None, "tensor"),
            P("dp", "tensor"),
            P("dp", None),
            P("dp", None),
            P("dp", None),
        ),
        out_specs=(P("dp", "tensor"), P("dp", "tensor"), P("dp", "tensor")),
        check_vma=False,
    )
```

```python
import functools

import jax
import jax.numpy as jnp
from jax import lax
from jax.experimental import pallas as pl
from jax.experimental.pallas import tpu as pltpu
from jax.sharding import PartitionSpec as P

MESH = pl.DeviceIdType.MESH
F32 = jnp.float32
BF16 = jnp.bfloat16
EARLY = 2
PARTS = 1


def split3(a):
    hi = a.astype(BF16)
    rest = a - hi.astype(F32)
    mid = rest.astype(BF16)
    low = (rest - mid.astype(F32)).astype(BF16)
    return jnp.concatenate([hi, mid, low], axis=0)


def tdot(a, b):
    return lax.dot_general(a, b, (((0,), (0,)), ((), ())), preferred_element_type=F32)


def plan(nu, ns, early):
    steps = []
    for u in range(nu):
        lead = u < nu // 2
        own = 2.0 + 0.2 * u if lead else (3.05 + 0.05 * (u - nu // 2) if u < nu - 2 else 5.15 + 0.05 * (u + 2 - nu))
        steps.append((own, "own", u))
        if u < early:
            steps.append((early + 0.1 + 0.25 * u, "prep", u))
            arrived = early + 0.2 + 0.25 * u
        else:
            arrived = u + 1.0
        steps.append((arrived, "other", u))
        if u % 2:
            sent = max(own + 0.01, 3.05 + 0.67 * (u - 1))
            steps.append((sent, "own_out", u))
            steps.append((min(sent + 1.3, nu - 1.04) if u < nu - 1 else sent + 1.3, "own_pass", u))
            sent = max(arrived + 0.01, 3.7 + 0.66 * (u - 1))
            if u < nu - 1:
                steps.append((sent, "other_out", u))
            steps.append((min(sent + 1.2, nu - 1.05) if u < nu - 1 else sent + 0.1, "other_pass", u))
        if (u + 1) % (2 * ns) == 0 and u < nu - 1:
            steps.append((arrived + 1.5, "attn", u // (2 * ns)))
        if u == nu - 2:
            steps.append((arrived - 0.6, "attn_part", range(nu - 2 * ns, u)))
            steps.append((arrived + 0.2, "attn_part1", [u]))
        if u == nu - 1:
            steps.append((arrived + 1.0, "attn_part0", [u - 1]))
            steps.append((arrived + 1.1, "attn_part", [u]))
    steps.append((4.2, "own_attn", 0))
    steps.append((4.25, "memory", 0))
    return [step[1:] for step in sorted(steps, key=lambda step: step[0])]


def kernel(
    n, early, attn_hbm, w_hbm, g_hbm, rwt_hbm, gate_hbm, wpos_hbm, out_attn, out_w, out_mem,
    rwt, gate, wpos, g, attn, w, attn_p, za, zb, zp, zpx, acc, onehot, mask, grow, rows, early_rows, rows_x, local, after,
    gpad, grecv, lrecv, asend, arecv, ysend, yrecv, kept, zsend, zpass, zrecv, mine,
    small_sem, g_sem, attn_sem, w_sem, x_s, x_r, gt_s, gt_r, l_s, l_r, a_s, a_r, r_s, r_r, t_s, t_r,
    p_s, p_r, q_s, q_r, y_s, y_r, z_s, v_r, z_r,
):
    d = lax.axis_index("dp")
    t = lax.axis_index("tensor")
    c = lax.rem(d, 2)
    y = lax.rem(d // 2, 2)
    z = d // 4
    nz = n // 4
    seg, half = g.shape
    hd = attn.shape[1]
    slots = rwt.shape[0]
    bw = 2 * half // n
    lw = half // n
    zh = nz // 2
    sub = mask.shape[1]
    ns = bw // sub
    nu = 2 * zh * ns
    oh = 1 - t
    pd = d + 1 - 2 * c
    partner = (pd, t)
    xpeer = (d, oh)
    ypeer = (d + 2 - 4 * y, t)
    tile = 256

    def remote(src, dst, ss, rs, dev):
        return pltpu.make_async_remote_copy(
            src_ref=src, dst_ref=dst, send_sem=ss, recv_sem=rs, device_id=dev, device_id_type=MESH
        )

    def all_sent(ref, sem):
        remote(ref, ref, sem, sem, xpeer).wait_send()

    def all_here(ref, sem):
        remote(ref, ref, sem, sem, xpeer).wait_recv()

    def peer(o):
        return lax.rem(d + o, n)

    barrier = pltpu.get_barrier_semaphore()
    for o in range(1, n):
        pl.semaphore_signal(barrier, inc=1, device_id=(peer(o), t), device_id_type=MESH)
    pl.semaphore_signal(barrier, inc=1, device_id=xpeer, device_id_type=MESH)
    pl.semaphore_signal(barrier, inc=1, device_id=(pd, oh), device_id_type=MESH)

    smalls = [
        pltpu.make_async_copy(src, dst, small_sem.at[i])
        for i, (src, dst) in enumerate(((rwt_hbm, rwt), (gate_hbm, gate), (wpos_hbm, wpos)))
    ]
    for copy in smalls:
        copy.start()
    gcopy = pltpu.make_async_copy(g_hbm, g, g_sem)
    gcopy.start()
    attncopy = pltpu.make_async_copy(attn_hbm, attn, attn_sem)
    pl.semaphore_wait(barrier, n + 1)

    def is_other(u):
        return u % 2 == 0

    def level(h, r):
        return r + h * (zh - 1 - 2 * r)

    def cols(h, u, par):
        yd = 1 - y if is_other(u) else y
        j = 2 * level(h, u // (2 * ns)) + yd
        piece = u % (2 * ns) // 2
        return pl.ds(pl.multiple_of((2 * j + par) * bw + piece * sub, sub), sub)

    def wide(h, r):
        return pl.multiple_of(4 * level(h, r) * bw, 4 * bw)

    xa, xb = [], []
    for u in range(nu):
        mine_at, part_at = cols(t, u, c), cols(t, u, 1 - c)
        src = g if u < early else za
        xa.append(remote(src.at[:, mine_at], zb.at[:, mine_at], x_s.at[0], x_r.at[u], xpeer))
        if u < early:
            xb.append(remote(src.at[:, part_at], zb.at[:, part_at], x_s.at[1], x_r.at[u], xpeer))
        else:
            xb.append(remote(src.at[:, part_at], zpx.at[u], x_s.at[1], x_r.at[u], (pd, oh)))
    gcopy.wait()
    for u in range(early):
        xb[u].start()
        xa[u].start()

    for copy in smalls:
        copy.wait()
    gpad[...] = jnp.zeros_like(gpad)
    gpad[:, :slots] = gate[...].T
    grecv[0] = gpad[...]
    gcopies = [remote(gpad, grecv.at[o], gt_s, gt_r, (peer(o), t)) for o in range(1, n)]
    for copy in gcopies:
        copy.start()
    wcopy = pltpu.make_async_copy(w_hbm, w, w_sem)
    tcopy = remote(attn_hbm, attn_p, t_s, t_r, partner)
    three = split3(rwt[...])

    def local_step(i, _):
        at = pl.ds(pl.multiple_of(i * tile, tile), tile)
        r = jnp.dot(three, g[:, at], preferred_element_type=F32)
        local[:, at] = r[:slots] + r[slots : 2 * slots] + r[2 * slots :]
        return 0

    lax.fori_loop(0, half // tile, local_step, 0)

    def slab(o):
        return pl.ds(pl.multiple_of(peer(o) * lw, lw), lw)

    lcopies = [
        remote(local.at[:, slab(o)], lrecv.at[o], l_s, l_r, (peer(o), t)) for o in range(1, n)
    ]
    for copy in lcopies:
        copy.start()
    lrecv[0] = local[:, slab(0)]
    attncopy.start()
    tcopy.start()

    place_of = lax.broadcasted_iota(jnp.int32, (seg, slots), 0)
    hit = jnp.where(place_of == wpos[...], 1.0, 0.0)
    onehot[...] = hit.astype(BF16)
    mask[...] = jnp.broadcast_to(jnp.sum(hit, axis=1, keepdims=True), mask.shape)

    def row_step(i, _):
        at = pl.ds(pl.multiple_of(i * tile, tile), tile)
        grow[:, at] = tdot(onehot[...], g[:, at])
        return 0

    lax.fori_loop(0, half // tile, row_step, 0)
    others = pl.ds(1, n - 1)
    all_here(grecv.at[others], gt_r)
    all_here(lrecv.at[others], l_r)

    def acopy(o, target):
        return remote(asend.at[o], arecv.at[o], a_s, a_r, (target, t))

    def sweep(i, carry):
        s = n - 1 - i
        slot = lax.rem(d - s + n, n)
        target = lax.rem(s - d + n, n)
        asend[target] = carry
        gates = grecv[slot]
        fresh = lrecv[slot]
        for k in range(slots):
            fresh = fresh + gates[:, k : k + 1] * carry[k : k + 1, :]

        @pl.when(target != 0)
        def _():
            acopy(target, s).start()

        return fresh

    lax.fori_loop(0, n, sweep, jnp.zeros((slots, lw), F32))
    wcopy.start()
    all_here(arecv.at[others], a_r)
    for o in range(n):
        src = lax.rem(d - o + n, n)
        at = pl.ds(pl.multiple_of(src * lw, lw), lw)
        got = arecv[o] if o else asend[0]
        after[:, at] = got
        rows[:, at] = (grow[:, at] + got).astype(BF16)
    for u in range(early):
        for k, at in enumerate((cols(t, u, 1 - c), cols(t, u, c))):
            early_rows[:, pl.ds((2 * u + k) * sub, sub)] = rows[:, at]
    rcopy = remote(early_rows, rows_x, r_s, r_r, xpeer)
    rcopy.start()

    def fix(src, new_rows, dst, at):
        picked = jnp.dot(onehot[...], new_rows, preferred_element_type=F32)
        dst[:, at] = jnp.where(mask[...] > 0.5, picked, src[:, at].astype(F32)).astype(BF16)

    pcopies = [
        remote(za.at[:, cols(t, u, 1 - c)], zp.at[u], p_s, p_r.at[u // (nu - 2)], partner) for u in range(nu)
    ]
    qcopies = []
    groups = [[u] for u in range(early)]
    groups += [list(range(max(early, 2 * ns * r), 2 * ns * (r + 1))) for r in range(zh)]
    groups[-1] = groups[-1][:-2]
    groups += [[nu - 2], [nu - 1]]
    group_of = {u: k for k, group in enumerate(groups) for u in group}
    for u in range(nu):
        got = q_r.at[group_of[u]]
        if u < early:
            qcopies.append(remote(zb.at[:, cols(oh, u, 1 - c)], zpx.at[u], q_s, got, partner))
        else:
            qcopies.append(remote(zpx.at[u], zb.at[:, cols(oh, u, c)], q_s, got, partner))

    def blocks(count):
        return zpx.at[pl.ds(0, count)]

    def q_here(u):
        all_here(blocks(len(groups[group_of[u]])), q_r.at[group_of[u]])

    def fix_own(u):
        for at in (cols(t, u, 1 - c), cols(t, u, c)):
            fix(g, rows[:, at], za, at)
        pcopies[u].start()
        pair = [] if u < early or u == nu - 2 else [u] if u < nu - 2 else [nu - 2, nu - 1]
        if pair:

            @pl.when(c == 0)
            def _():
                for v in pair:
                    xa[v].start()
                for v in pair:
                    xb[v].start()

            @pl.when(c == 1)
            def _():
                for v in pair:
                    xb[v].start()
                for v in pair:
                    xa[v].start()

    for u in [*range(early, min(early + 2, nu)), *range(early), *range(early + 2, nu)]:
        fix_own(u)


    def slot_of(own, u):
        return (0 if own else nu // 2) + u // 2

    def product(own, u, ht):
        zr, zq, at = (za, zp, cols(t, u, c)) if own else (zb, zpx, cols(oh, u, c))
        return tdot(zr[:, at], attn[:, ht]) + tdot(zq[u], attn_p[:, ht])

    def grad_block(own, u):
        slot = slot_of(own, u)

        def step(m, _):
            ht = pl.ds(pl.multiple_of(m * tile, tile), tile)
            r = product(own, u, ht)
            if is_other(u):
                ysend[slot, :, ht] = r.astype(BF16)
            else:
                kept[slot, :, ht] = r
            return 0

        lax.fori_loop(0, hd // tile, step, 0)
        if is_other(u):
            ycopy(slot, every, slot).start()

    every = pl.ds(0, hd)

    def ycopy(slot, ht, k):
        return remote(ysend.at[slot, :, ht], yrecv.at[slot, :, ht], y_s, y_r.at[k], ypeer)

    def last_sent_block(u):
        slot = slot_of(False, u)
        for k in range(2):
            ht = pl.ds(k * (hd // 2), hd // 2)
            ysend[slot, :, ht] = product(False, u, ht).astype(BF16)
            ycopy(slot, ht, slot + k).start()

    outer = (z == 0) | (z == nz - 1)
    low = z < zh
    inner_z = jnp.where(low, zh - 1, zh)

    def place(own, u):
        zd = zh * (t if own else oh) + level(t if own else oh, u // (2 * ns))
        across = (zd < zh) != low
        return slot_of(own, u), u % (2 * ns) // 2, zd, zd == z, across

    def at_chip(zt):
        return (zt * 4 + 2 * y + c, t)

    def to_relay(slot, ht, k):
        return remote(
            zsend.at[slot, :, ht], zpass.at[slot, :, ht], z_s, v_r.at[slot + k], at_chip(inner_z)
        )

    def to_home(slot, piece, zd, ht, kind):
        return remote(
            zsend.at[slot, :, ht], zrecv.at[kind, piece, :, ht], z_s, z_r.at[kind, piece], at_chip(zd)
        )

    def first_stage(own, u, total, ht, k):
        slot, piece, zd, at_home, across = place(own, u)

        @pl.when(at_home)
        def _():
            mine[piece, :, ht] = total

        @pl.when(across & jnp.logical_not(outer))
        def _():
            kept[slot, :, ht] = total

        @pl.when(across & outer)
        def _():
            zsend[slot, :, ht] = total.astype(BF16)
            to_relay(slot, ht, k).start()

        @pl.when(jnp.logical_not(across | at_home))
        def _():
            zsend[slot, :, ht] = total.astype(BF16)
            to_home(slot, piece, zd, ht, 1).start()

    def second_stage(own, u, ht, k):
        slot, piece, zd, _, across = place(own, u)

        @pl.when(across & jnp.logical_not(outer))
        def _():
            to_relay(slot, ht, k).wait_recv()
            zsend[slot, :, ht] = (kept[slot, :, ht] + zpass[slot, :, ht].astype(F32)).astype(BF16)
            to_home(slot, piece, zd, ht, 0).start()

    def to_owner(own, u):
        slot = slot_of(own, u)
        ycopy(slot, every, slot).wait_recv()
        first_stage(own, u, kept[slot] + yrecv[slot].astype(F32), every, 0)

    def last_block(u):
        slot = slot_of(False, u)
        for k in range(4):
            ht = pl.ds(k * (hd // 4), hd // 4)
            total = product(False, u, ht)
            if k % 2 == 0:
                at = pl.ds(k // 2 * (hd // 2), hd // 2)
                ycopy(slot, at, slot + k // 2).wait_recv()
            first_stage(False, u, total + yrecv[slot, :, ht].astype(F32), ht, k)

    def pass_on(own, u):
        if not own and u == nu - 1:
            for k in range(4):
                second_stage(own, u, pl.ds(k * (hd // 4), hd // 4), k)
        else:
            second_stage(own, u, every, 0)

    def own_attn():
        wcopy.wait()

        def step(m, _):
            at = pl.ds(pl.multiple_of(m * tile, tile), tile)
            k = pl.ds(pl.multiple_of(t * half, half), half)
            acc[:, at] = jnp.dot(za[...], w[k, at], preferred_element_type=F32)
            return 0

        lax.fori_loop(0, hd // tile, step, 0)

    def other_attn(r):
        from_at = wide(oh, r)
        if 2 * ns * (r + 1) > early:
            q_here(2 * ns * (r + 1) - 1)

        def step(m, _):
            at = pl.ds(pl.multiple_of(m * tile, tile), tile)
            k = pl.ds(pl.multiple_of(oh * half + from_at, 4 * bw), 4 * bw)
            total = acc[:, at] + jnp.dot(
                zb[:, pl.ds(from_at, 4 * bw)], w[k, at], preferred_element_type=F32
            )
            acc[:, at] = total
            return 0

        lax.fori_loop(0, hd // tile, step, 0)

    def part_attn(units):
        q_here(units[-1])
        places = [cols(oh, u, par) for u in units for par in range(2)]

        def step(m, _):
            at = pl.ds(pl.multiple_of(m * tile, tile), tile)
            lhs = jnp.concatenate([zb[:, k] for k in places], axis=1)
            rhs = jnp.concatenate(
                [w[pl.ds(pl.multiple_of(oh * half + k.start, sub), sub), at] for k in places], axis=0
            )
            total = acc[:, at] + jnp.dot(lhs, rhs, preferred_element_type=F32)
            if nu - 1 in units:
                out_attn[:, at] = total.astype(BF16)
            else:
                acc[:, at] = total
            return 0

        lax.fori_loop(0, hd // tile, step, 0)

    def memory():
        gates = gpad[...]

        def step(i, _):
            at = pl.ds(pl.multiple_of(i * tile, tile), tile)
            fresh = local[:, at]
            carry = after[:, at]
            for k in range(slots):
                fresh = fresh + gates[:, k : k + 1] * carry[k : k + 1, :]
            out_mem[:, at] = fresh
            return 0

        lax.fori_loop(0, half // tile, step, 0)

    attncopy.wait()
    tcopy.wait_recv()
    for kind, u in plan(nu, ns, early):
        if kind == "own":
            if u == 0:
                all_here(blocks(nu - 2), p_r.at[0])
            if u == nu - 2:
                all_here(blocks(2), p_r.at[1])
            grad_block(True, u)
        elif kind == "prep":
            if u == 0:
                rcopy.wait_recv()
            all_here(blocks(2), x_r.at[u])
            fix(zb, rows_x[:, pl.ds(2 * u * sub, sub)], zb, cols(oh, u, 1 - c))
            qcopies[u].start()
            fix(zb, rows_x[:, pl.ds((2 * u + 1) * sub, sub)], zb, cols(oh, u, c))
        elif kind == "other":
            if u < early:
                q_here(u)
            else:
                all_here(blocks(2), x_r.at[u])
                qcopies[u].start()
            if u < nu - 2:
                grad_block(False, u)
            elif u < nu - 1:
                last_sent_block(u)
            else:
                last_block(u)
        elif kind == "own_out":
            to_owner(True, u)
        elif kind in ("own_pass", "other_pass"):
            pass_on(kind == "own_pass", u)
        elif kind == "other_out":
            to_owner(False, u)
        elif kind == "own_attn":
            own_attn()
        elif kind == "attn":
            other_attn(u)
        elif kind == "attn_part":
            part_attn(u)
        elif kind in ("attn_part0", "attn_part1"):

            @pl.when(c == int(kind[-1]))
            def _(u=u):
                part_attn(u)

        else:
            memory()

    for piece in range(ns):
        total = mine[piece]
        for kind in range(2):
            to_home(0, piece, z, every, kind).wait_recv()
            total = total + zrecv[kind, piece].astype(F32)
        out_w[pl.ds(piece * sub, sub), :] = total

    all_sent(zp, x_s.at[0])
    all_sent(zp, x_s.at[1])
    all_sent(zp, p_s)
    all_sent(zp, q_s)
    all_sent(grecv.at[others], gt_s)
    all_sent(lrecv.at[others], l_s)
    all_sent(arecv.at[others], a_s)
    rcopy.wait_send()
    all_sent(yrecv, y_s)
    all_sent(zsend.at[pl.ds(0, nu - ns)], z_s)
    tcopy.wait_send()


def settle_kernel(a, b, m, out_a, out_b, out_m, sems):
    copies = []
    for src, dst, parts in ((a, out_a, PARTS), (b, out_b, PARTS), (m, out_m, 1)):
        rows = src.shape[0] // parts
        for i in range(parts):
            at = pl.ds(i * rows, rows)
            copies.append(pltpu.make_async_copy(src.at[at], dst.at[at], sems.at[len(copies)]))
    for copy in copies:
        copy.start()
    for copy in copies:
        copy.wait()


def settled(outs):
    return pl.pallas_call(
        settle_kernel,
        out_shape=tuple(jax.ShapeDtypeStruct(o.shape, o.dtype) for o in outs),
        in_specs=[pl.BlockSpec(memory_space=pltpu.VMEM)] * 3,
        out_specs=tuple([pl.BlockSpec(memory_space=pl.ANY)] * 3),
        scratch_shapes=[pltpu.SemaphoreType.DMA((2 * PARTS + 1,))],
    )(*[pltpu.with_memory_space_constraint(o, pltpu.VMEM) for o in outs])


def fused(n, attn_out, out_proj_t, grad_out, read_weights, memory_gate, write_pos):
    seg, half = grad_out.shape
    hd = attn_out.shape[1]
    slots = write_pos.shape[1]
    depth = out_proj_t.shape[0]
    bw, lw, nz = depth // n, half // n, n // 4
    sub = 128
    ns = bw // sub
    nu = nz * ns
    zh = nz // 2
    early = EARLY
    V = pltpu.VMEM
    D = pltpu.SemaphoreType.DMA
    vmem = pl.BlockSpec(memory_space=pltpu.VMEM)
    outs = pl.pallas_call(
        functools.partial(kernel, n, early),
        out_shape=(V((seg, hd), BF16), V((bw, hd), F32), V((slots, half), F32)),
        in_specs=[pl.BlockSpec(memory_space=pl.ANY)] * 6,
        out_specs=(vmem, vmem, vmem),
        scratch_shapes=[
            V((slots, seg), F32),
            V((slots, slots), F32),
            V((1, slots), jnp.int32),
            V((seg, half), BF16),
            V((seg, hd), BF16),
            V((depth, hd), BF16),
            V((seg, hd), BF16),
            V((seg, half), BF16),
            V((seg, half), BF16),
            V((nu, seg, sub), BF16),
            V((nu, seg, sub), BF16),
            V((seg, hd), F32),
            V((seg, slots), BF16),
            V((seg, sub), F32),
            V((slots, half), F32),
            V((slots, half), BF16),
            V((slots, 2 * early * sub), BF16),
            V((slots, 2 * early * sub), BF16),
            V((slots, half), F32),
            V((slots, half), F32),
            V((slots, 128), F32),
            V((n, slots, 128), F32),
            V((n, slots, lw), F32),
            V((n, slots, lw), F32),
            V((n, slots, lw), F32),
            V((nu, sub, hd), BF16),
            V((nu, sub, hd), BF16),
            V((nu, sub, hd), F32),
            V((nu, sub, hd), BF16),
            V((nu, sub, hd), BF16),
            V((2, ns, sub, hd), BF16),
            V((ns, sub, hd), F32),
            D((3,)),
            D,
            D,
            D,
            D((2,)),
            D((nu,)),
            D,
            D,
            D,
            D,
            D,
            D,
            D,
            D,
            D,
            D,
            D,
            D((2,)),
            D,
            D((early + zh + 2,)),
            D,
            D((nu - 1 + hd // 256,)),
            D,
            D((nu - 1 + hd // 256,)),
            D((2, ns)),
        ],
        compiler_params=pltpu.CompilerParams(
            collective_id=0, has_side_effects=True, vmem_limit_bytes=52 * 1024 * 1024
        ),
    )(attn_out, out_proj_t, grad_out, read_weights.T, memory_gate, write_pos)
    return settled(outs)


def plain(attn_out, out_proj_t, grad_out, read_weights, memory_gate, write_pos):
    high = lax.Precision.HIGHEST
    seg_len = attn_out.shape[0]
    slots = write_pos.shape[1]
    gate_at_step = memory_gate.T
    dy_cols = grad_out.astype(jnp.float32)
    local = jnp.dot(read_weights.T, dy_cols, precision=high, preferred_element_type=jnp.float32)
    all_gates, all_terms = (
        lax.all_gather(gate_at_step, "dp", axis=0, tiled=True),
        lax.all_gather(local, "dp", axis=0, tiled=True),
    )
    count = lax.axis_size("dp")
    mine = lax.axis_index("dp")

    def sweep(step, carry):
        which = (count - 1 - step).astype(jnp.int32)
        gate = lax.dynamic_slice_in_dim(all_gates, which * slots, slots, 0)
        term = lax.dynamic_slice_in_dim(all_terms, which * slots, slots, 0)
        fresh = jnp.dot(gate, carry, precision=high, preferred_element_type=jnp.float32) + term
        return jnp.where(which > mine, fresh, carry)

    after = lax.fori_loop(0, count, sweep, jnp.zeros_like(local))
    grad_memory = (
        jnp.dot(gate_at_step, after, precision=high, preferred_element_type=jnp.float32) + local
    )
    places = jnp.arange(seg_len, dtype=jnp.int32)
    onehot = (places[:, None] == write_pos[0][None, :]).astype(jnp.float32)
    written = jnp.dot(onehot, after, precision=high, preferred_element_type=jnp.float32)
    grad_z = (dy_cols + written).astype(jnp.bfloat16)
    full_z = lax.all_gather(grad_z, "tensor", axis=1, tiled=True)
    grad_attn = jnp.dot(full_z, out_proj_t, preferred_element_type=jnp.float32).astype(jnp.bfloat16)
    term = lax.dot_general(
        full_z, attn_out, (((0,), (0,)), ((), ())), preferred_element_type=jnp.float32
    )
    grad_weight = lax.psum_scatter(term, "dp", scatter_dimension=0, tiled=True)
    return (grad_attn, grad_weight, grad_memory)


def solution(mesh):
    n = mesh.shape["dp"]
    parts = mesh.shape["tensor"]

    def body(attn_out, out_proj_t, grad_out, read_weights, memory_gate, write_pos):
        half, hd = grad_out.shape[1], attn_out.shape[1]
        fits = (
            parts == 2
            and n // 4 == 4
            and half % (n * 128) == 0
            and half % 256 == 0
            and hd % 256 == 0
            and out_proj_t.shape[0] <= 4096
        )
        args = (attn_out, out_proj_t, grad_out, read_weights, memory_gate, write_pos)
        return fused(n, *args) if fits else plain(*args)

    return jax.shard_map(
        body,
        mesh=mesh,
        in_specs=(
            P("dp", "tensor"),
            P(None, "tensor"),
            P("dp", "tensor"),
            P("dp", None),
            P("dp", None),
            P("dp", None),
        ),
        out_specs=(P("dp", "tensor"), P("dp", "tensor"), P("dp", "tensor")),
        check_vma=False,
    )
```
